256 devices in a mesh: dp: 64 (over x, y_hi, z), mp: 4 (over y_lo, core).
Axes of the slice: x: 4, y: 4 (y_hi: 2, y_lo: 2; y = y_hi * 2 + y_lo), z: 8, core: 2. Of those that a mesh axis runs over, the one named last changes fastest.
Arguments:
- z_star: bfloat16 [64, 257, 1280], P('dp', None, 'mp'), may hold values from -24 to 24
- cotangent: float32 [64, 257, 1280], P('dp', None, 'mp'), may hold values from -16 to 16
- w_qkv: bfloat16 [3, 1280, 1280], P(None, None, 'mp'), may hold values from -1 to 1
- w_out: bfloat16 [1280, 1280], P('mp'), may hold values from -0.15625 to 0.15625
Outputs:
- implicit: float32 [64, 257, 1280], P('dp', None, 'mp')
- grad_qkv: float32 [3, 1280, 1280], P(None, 'dp', 'mp')
- grad_out: float32 [1280, 1280], P('mp', 'dp')
The draws below stay inside these ranges and needn't reach their ends.
All inputs are finite; a program needn't handle non-finite values.
Results may differ from the reference program's by a relative error of at most 0.0091.
Values may be sent and summed in bfloat16 or wider, within the bound.
No kernel may reach another device: no remote copies, remote signals or barrier semaphores. Data moves between devices by JAX's collectives and lax.ppermute only.
A program may use at most 128 MiB of HBM per device.

```python
import math
import jax
import jax.numpy as jnp
from jax import lax

D = 1280
HEADS = 16
HD = 80
S = 257
IMG_DEV = 1
TERMS = 3
HH = 1280
IMAGES = 64
N_DP = 64


def boosted(key):
    shuffled = jax.random.permutation(jax.random.fold_in(key, 7), N_DP)
    owners = shuffled[jnp.arange(IMAGES) // IMG_DEV]
    blocks = jnp.arange(D) // (D // N_DP)
    return jnp.where(blocks[None, :] == owners[:, None], 3.0, 1.0).astype(jnp.float32)


def draw_z_star(key, part):
    scales = boosted(key)
    values = jnp.clip(jax.random.normal(jax.random.fold_in(key, 1), (IMAGES, S, D), jnp.float32), -6.0, 6.0)
    return (values * scales[:, None, :]).astype(jnp.bfloat16)


def draw_w_qkv(key, part):
    values = jnp.clip(jax.random.normal(jax.random.fold_in(key, 11), (3, D, HEADS * HD), jnp.float32), -6.0, 6.0) / math.sqrt(D)
    return values.astype(jnp.bfloat16)


def strengthened(values, own_key, source, target, shards_of, factor):
    owner, partner = [(jnp.arange(values.shape[dim]) // (values.shape[dim] // shards_of)).reshape([-1 if axis == dim else 1 for axis in range(values.ndim)]) for dim in (source, target)]
    chosen = jax.random.permutation(own_key, shards_of)[partner]
    strong = (owner == chosen) | (owner == (partner + shards_of // 2) % shards_of)
    return jnp.where(strong, factor * values, values)


def level_of(key, dims, shards, least, largest):
    def one(dim, parts):
        draws = jax.random.uniform(jax.random.fold_in(jax.random.fold_in(key, 6), dim), (parts,), jnp.float32, least / len(shards), largest / len(shards))
        return jnp.repeat(jnp.exp(draws), dims[dim] // parts).reshape((-1,) + (1,) * (len(dims) - dim - 1))

    gain = one(*shards[0])
    for cut in shards[1:]:
        gain = gain * one(*cut)
    return gain


def scatter_about(stream_key, shape, scale, bound, split=(), dtype=jnp.bfloat16):
    drawn = scale * jax.random.normal(stream_key, shape, jnp.float32)
    if split:
        drawn = drawn * level_of(stream_key, shape, split, -0.22, 0.18)
    return jnp.clip(drawn, -bound, bound).astype(dtype)


def bell_draw_with(key, shape, scale, reach, pieces, heavy, kind=jnp.bfloat16):
    values = scale * jax.random.normal(key, shape, jnp.float32)
    if pieces:
        values = values * level_of(key, shape, pieces, -0.22, 0.18)
    return jnp.clip(strengthened(values, jax.random.fold_in(key, 3), *heavy), -reach, reach).astype(kind)


def setup_inputs(seed: int = 0) -> dict:
    key_of = jax.random.split(jax.random.key(seed), 5)
    z_star = draw_z_star(jax.random.fold_in(key_of[4], 71), 0)
    cotangent = bell_draw_with(key_of[1], (IMAGES, S, D), 1.0, 16.0, ((0, 64), (2, 4)), (0, 2, 64, 4.0), jnp.float32)
    w_qkv = draw_w_qkv(jax.random.fold_in(key_of[4], 71), 0)
    w_out = scatter_about(key_of[3], (HH, D), HH ** -0.5, 0.15625, ((0, 4),))
    return dict(z_star=z_star, cotangent=cotangent, w_qkv=w_qkv, w_out=w_out)


epsilon = 1e-06

def layer_norm(z_block):
    values = z_block.astype(jnp.float32)
    centred = values - lax.optimization_barrier(jnp.mean(values, axis=-1, keepdims=True))
    inv_std = lax.rsqrt(lax.optimization_barrier(jnp.mean(centred * centred, axis=-1, keepdims=True)) + epsilon)
    return (centred * inv_std, inv_std)

def reference(z_star, cotangent, w_qkv, w_out):
    score_scale = HD ** (-0.5)
    features = HEADS * HD

    def one_block(running_grads, inputs):
        grad_q, grad_o = running_grads
        z_block, cot_block = inputs
        images, tokens, model_width = z_block.shape
        normal_f, inv_std = layer_norm(z_block)
        normal_b = normal_f.astype(jnp.bfloat16)
        flattened = normal_b.reshape(-1, model_width)

        def project(slot_index):
            result = jnp.dot(flattened, w_qkv[slot_index], preferred_element_type=jnp.float32)
            return result.astype(jnp.bfloat16).reshape(images, tokens, HEADS, HD)
        queries = project(0)
        key_vecs = project(1)
        val_vecs = project(2)
        scores = jnp.einsum('bqhe,bkhe->bhqk', queries.astype(jnp.float32), key_vecs.astype(jnp.float32)) * score_scale
        attn_probs = jax.nn.softmax(scores, axis=-1)
        probs_b = attn_probs.astype(jnp.bfloat16)
        attended = jnp.einsum('bhqk,bkhe->bqhe', probs_b.astype(jnp.float32), val_vecs.astype(jnp.float32))
        attended = attended.astype(jnp.bfloat16).reshape(-1, features)
        current = cot_block
        running = cot_block
        for term_index in range(TERMS):
            cot_b = current.astype(jnp.bfloat16).reshape(-1, model_width)
            att_grad = jnp.dot(cot_b, w_out.T, preferred_element_type=jnp.float32)
            att_grad = att_grad.astype(jnp.bfloat16).reshape(images, tokens, HEADS, HD)
            grad_o = grad_o + jnp.dot(attended.T, cot_b, preferred_element_type=jnp.float32)
            prob_grad = jnp.einsum('bqhe,bkhe->bhqk', att_grad.astype(jnp.float32), val_vecs.astype(jnp.float32))
            rowdot = lax.optimization_barrier(jnp.sum(attn_probs * prob_grad, axis=-1, keepdims=True))
            score_grad = (attn_probs * (prob_grad - rowdot) * score_scale).astype(jnp.bfloat16)
            q_grad = jnp.einsum('bhqk,bkhe->bqhe', score_grad.astype(jnp.float32), key_vecs.astype(jnp.float32)).astype(jnp.bfloat16)
            k_grad = jnp.einsum('bhqk,bqhe->bkhe', score_grad.astype(jnp.float32), queries.astype(jnp.float32)).astype(jnp.bfloat16)
            v_grad = jnp.einsum('bhqk,bqhe->bkhe', probs_b.astype(jnp.float32), att_grad.astype(jnp.float32)).astype(jnp.bfloat16)
            qkv_grads = [item.reshape(-1, features) for item in (q_grad, k_grad, v_grad)]
            grad_q = grad_q + jnp.stack([jnp.dot(flattened.T, item, preferred_element_type=jnp.float32) for item in qkv_grads])
            if term_index + 1 < TERMS:
                in_grad = jnp.dot(qkv_grads[0], w_qkv[0].T, preferred_element_type=jnp.float32)
                in_grad = in_grad + jnp.dot(qkv_grads[1], w_qkv[1].T, preferred_element_type=jnp.float32)
                in_grad = in_grad + jnp.dot(qkv_grads[2], w_qkv[2].T, preferred_element_type=jnp.float32)
                in_grad = in_grad.reshape(images, tokens, model_width)
                row_mean = lax.optimization_barrier(jnp.mean(in_grad, axis=-1, keepdims=True))
                row_dot = lax.optimization_barrier(jnp.mean(in_grad * normal_f, axis=-1, keepdims=True))
                current = (in_grad - row_mean - normal_f * row_dot) * inv_std
                running = running + current
        return ((grad_q, grad_o), running)
    blocks = IMAGES // IMG_DEV
    z_blocks = z_star.reshape(blocks, IMG_DEV, S, D)
    cot_blocks = cotangent.reshape(blocks, IMG_DEV, S, D)
    start = (jnp.zeros((3, D, features), jnp.float32), jnp.zeros((features, D), jnp.float32))
    (grad_q, grad_o), totals = lax.scan(one_block, start, (z_blocks, cot_blocks))
    factor = 1.0 / math.sqrt(IMAGES * S)
    return (totals.reshape(IMAGES, S, D), grad_q * factor, grad_o * factor)
```

```python
import math

import jax
import jax.numpy as jnp
from jax import lax
from jax.sharding import Mesh
from jax.sharding import PartitionSpec as P

HD = 80
TERMS = 3
AXES = ("x", "yh", "z", "yl", "c")
DP = ("x", "yh", "z")
MP = ("yl", "c")
SWAP = [(0, 1), (1, 0)]

epsilon = 1e-06
f32 = jnp.float32
bf16 = jnp.bfloat16


def both_chips(mine, yl):
    theirs = lax.ppermute(mine, "yl", SWAP)
    first = jnp.where(yl == 0, mine, theirs)
    second = jnp.where(yl == 0, theirs, mine)
    return jnp.concatenate([first, second], axis=-1)


def gathered(mine, yl):
    own = both_chips(mine, yl)
    return own, lax.ppermute(own, "c", SWAP)


def summed(own, other):
    chip = own.astype(f32) + lax.ppermute(other.astype(bf16), "c", SWAP).astype(f32)
    chip = chip.astype(bf16)
    whole = chip.astype(f32) + lax.ppermute(chip, "yl", SWAP).astype(f32)
    whole = whole.astype(bf16)
    return whole, lax.ppermute(whole, "c", SWAP)


def shift(n, by):
    return [(i, (i + by) % n) for i in range(n)]


def sum_x(parts):
    n = lax.axis_size("x")
    i = lax.axis_index("x")
    take = lambda j: lax.dynamic_index_in_dim(parts, lax.rem(j, n), 0, keepdims=False)
    got = [lax.ppermute(take(i + by), "x", shift(n, by)) for by in range(1, n)]
    out = take(i).astype(f32)
    for g in got:
        out = out + g.astype(f32)
    return out.astype(bf16)


def sum_yh(parts):
    i = lax.axis_index("yh")
    take = lambda j: lax.dynamic_index_in_dim(parts, j, 0, keepdims=False)
    got = lax.ppermute(take(1 - i), "yh", SWAP)
    return (take(i).astype(f32) + got.astype(f32)).astype(bf16)


def shards(z_star, cotangent, w_qkv, w_out):
    images, tokens, narrow = z_star.shape
    width = 4 * narrow
    heads = narrow // HD
    scale = HD ** (-0.5)
    yl = lax.axis_index("yl")
    c = lax.axis_index("c")

    def by_core(w, dim):
        dims = w.shape
        w = w.reshape(*dims[:dim], 2, 2, narrow, *dims[dim + 1 :])
        own = lax.dynamic_index_in_dim(w, c, dim + 1, keepdims=False)
        oth = lax.dynamic_index_in_dim(w, 1 - c, dim + 1, keepdims=False)
        flat = (*dims[:dim], 2 * narrow, *dims[dim + 1 :])
        return jnp.concatenate([own.reshape(flat), oth.reshape(flat)], axis=dim)

    def in_order(own, oth):
        a = jnp.where(c == 0, own, oth)
        b = jnp.where(c == 0, oth, own)
        a0, a1 = jnp.split(a, 2, axis=-1)
        b0, b1 = jnp.split(b, 2, axis=-1)
        return jnp.concatenate([a0, b0, a1, b1], axis=-1)

    wq = by_core(w_qkv, 1)
    wo = by_core(w_out, 1)

    z_own, z_oth = gathered(z_star[0], yl)
    t_own, t_oth = gathered(cotangent[0].astype(bf16), yl)
    values = jnp.concatenate([z_own, z_oth], axis=-1).astype(f32)
    centred = values - jnp.mean(values, axis=-1, keepdims=True)
    inv_std = lax.rsqrt(jnp.mean(centred * centred, axis=-1, keepdims=True) + epsilon)
    normal_f = centred * inv_std
    normal_b = normal_f.astype(bf16)

    def split(x):
        return x.astype(bf16).reshape(tokens, heads, HD)

    q, k, v = [split(jnp.dot(normal_b, wq[s], preferred_element_type=f32)) for s in range(3)]
    scores = jnp.einsum("qhe,khe->hqk", q, k, preferred_element_type=f32) * scale
    probs = jax.nn.softmax(scores, axis=-1)
    probs_b = probs.astype(bf16)
    attended = jnp.einsum("hqk,khe->qhe", probs_b, v, preferred_element_type=f32)
    attended = attended.astype(bf16).reshape(tokens, narrow)

    rows_rows = (((0,), (0,)), ((), ()))
    cols_cols = (((1,), (1,)), ((), ()))

    def attention_back(cot_b):
        att = split(lax.dot_general(cot_b, wo, cols_cols, preferred_element_type=f32))
        dp = jnp.einsum("qhe,khe->hqk", att, v, preferred_element_type=f32)
        dot = jnp.sum(probs * dp, axis=-1, keepdims=True)
        ds = (probs * (dp - dot) * scale).astype(bf16)
        gq = jnp.einsum("hqk,khe->qhe", ds, k, preferred_element_type=f32)
        gk = jnp.einsum("hqk,qhe->khe", ds, q, preferred_element_type=f32)
        gv = jnp.einsum("hqk,qhe->khe", probs_b, att, preferred_element_type=f32)
        return [g.astype(bf16).reshape(tokens, narrow) for g in (gq, gk, gv)]

    def input_back(grads, w):
        out = sum(
            lax.dot_general(g, w[s], cols_cols, preferred_element_type=f32)
            for s, g in enumerate(grads)
        )
        return out

    cot = jnp.concatenate([t_own, t_oth], axis=-1)
    total = cot.astype(f32)
    mine = 0.0
    for _ in range(TERMS - 1):
        grads = attention_back(cot)
        part = input_back(grads, wq)
        s_own, s_oth = summed(part[:, : 2 * narrow], part[:, 2 * narrow :])
        g = jnp.concatenate([s_own, s_oth], axis=-1).astype(f32)
        mean = jnp.mean(g, axis=-1, keepdims=True)
        dot = jnp.mean(g * normal_f, axis=-1, keepdims=True)
        term = (g - mean - normal_f * dot) * inv_std
        mine = mine + jnp.where(yl == 0, term[:, :narrow], term[:, narrow : 2 * narrow])
        total = total + term
        cot = term.astype(bf16)
    implicit = cotangent + mine[None]

    total_b = total.astype(bf16)
    grads = attention_back(total_b)
    x_n = in_order(normal_b[:, : 2 * narrow], normal_b[:, 2 * narrow :])
    x_t = in_order(total_b[:, : 2 * narrow], total_b[:, 2 * narrow :])

    def outer(a, b):
        return lax.dot_general(a, b, rows_rows, preferred_element_type=f32).astype(bf16)

    first = jnp.concatenate([outer(x_n, grads[0]), outer(x_n, grads[1])], axis=1)
    second = jnp.concatenate([outer(x_n, grads[2]), outer(x_t, attended)], axis=1)
    nx, ny, nz = [lax.axis_size(a) for a in DP]
    each = width // (nx * ny * nz)
    half = 2 * narrow
    first = sum_x(first.reshape(nx, ny * nz * each, half))
    first = sum_yh(first.reshape(ny, nz * each, half))
    second = sum_yh(jnp.moveaxis(second.reshape(nx, ny, nz * each, half), 1, 0))
    second = sum_x(second)
    both = jnp.concatenate([first, second], axis=1).reshape(nz, each, 2 * half)
    got = lax.all_to_all(both, "z", 0, 0, tiled=True)
    factor = 1.0 / math.sqrt(images * nx * ny * nz * tokens)
    got = jnp.sum(got.astype(f32), axis=0) * factor
    grad_qkv = jnp.stack([got[:, s * narrow : (s + 1) * narrow] for s in range(3)])
    return implicit, grad_qkv, got[:, 3 * narrow :].T


def solution(mesh):
    split = Mesh(mesh.devices.reshape(4, 2, 8, 2, 2), AXES)
    return jax.shard_map(
        shards,
        mesh=split,
        in_specs=(P(DP, None, MP), P(DP, None, MP), P(None, None, MP), P(MP, None)),
        out_specs=(P(DP, None, MP), P(None, DP, MP), P(MP, DP)),
        check_vma=False,
    )
```

```python
import functools
import math

import jax
import jax.numpy as jnp
from jax import lax
from jax.experimental import pallas as pl
from jax.experimental.pallas import tpu as pltpu
from jax.sharding import Mesh
from jax.sharding import PartitionSpec as P

HD = 80
AXES = ("x", "yh", "z", "yl", "c")
DP = ("x", "yh", "z")
MP = ("yl", "c")
SWAP = [(0, 1), (1, 0)]

epsilon = 1e-06
f32 = jnp.float32
bf16 = jnp.bfloat16
SCALE = HD ** (-0.5)
ROWS = (((0,), (0,)), ((), ()))
COLS = (((1,), (1,)), ((), ()))


def dot(a, b, dims=(((1,), (0,)), ((), ()))):
    return lax.dot_general(a, b, dims, preferred_element_type=f32)


def call(body, outs, ins, scratch=(), flops=0, name=None):
    vmem = pl.BlockSpec(memory_space=pltpu.VMEM)
    smem = pl.BlockSpec(memory_space=pltpu.SMEM)
    size = sum(math.prod(o.shape) * o.dtype.itemsize for o in list(outs) + list(ins))
    return pl.pallas_call(
        body,
        out_shape=outs,
        in_specs=[smem] + [vmem] * (len(ins) - 1),
        out_specs=[vmem] * len(outs),
        scratch_shapes=list(scratch),
        compiler_params=pltpu.CompilerParams(vmem_limit_bytes=28 * 2**20),
        cost_estimate=pl.CostEstimate(flops=flops, bytes_accessed=size, transcendentals=0),
        name=name,
    )(*ins)


def like(shape, dtype):
    return jax.ShapeDtypeStruct(shape, dtype)


def put_pieces(where, spot, pieces):
    narrow = pieces[0].shape[1]
    for g in range(4):

        @pl.when(where[0] == g)
        def _():
            for r, piece in zip((0, 2, 1, 3), pieces):
                at = (g ^ r) * narrow
                spot[:, at : at + narrow] = piece[...].astype(spot.dtype)


def put_halves(where, spot, own, oth):
    narrow = own.shape[1] // 2
    for c in range(2):

        @pl.when(where[1] == c)
        def _():
            for half, core in ((own, c), (oth, 1 - c)):
                for y in range(2):
                    at = (2 * y + core) * narrow
                    spot[:, at : at + narrow] = half[:, y * narrow : (y + 1) * narrow].astype(spot.dtype)


def forward_body(where, z0, zy, zc, zcy, w, normal_o, xt_o, inv_o, qkv_o, probs_o, att_o, zs):
    put_pieces(where, zs, (z0, zy, zc, zcy))
    width = zs.shape[1]
    narrow = w.shape[2]
    values = zs[...].astype(f32)
    centred = values - jnp.sum(values, axis=-1, keepdims=True) * (1.0 / width)
    inv = lax.rsqrt(jnp.sum(centred * centred, axis=-1, keepdims=True) * (1.0 / width) + epsilon)
    inv_o[...] = jnp.broadcast_to(inv, inv_o.shape)
    normal_o[...] = (centred * inv).astype(bf16)
    heads = narrow // HD
    for s in range(3):
        got = dot(normal_o[...], w[s]).astype(bf16)
        for h in range(heads):
            qkv_o[s * heads + h] = got[:, h * HD : (h + 1) * HD]
    for h in range(heads):
        scores = dot(qkv_o[h], qkv_o[heads + h], COLS) * SCALE
        top = jnp.max(scores, axis=-1, keepdims=True)
        e = jnp.exp(scores - top)
        probs = e / jnp.sum(e, axis=-1, keepdims=True)
        probs_o[h] = probs
        att_o[:, h * HD : (h + 1) * HD] = dot(probs.astype(bf16), qkv_o[2 * heads + h]).astype(bf16)
    xt_o[...] = normal_o[...].T


def attention_back(cot, w_out, qkv, probs, grads):
    narrow = w_out.shape[0]
    heads = narrow // HD
    att = dot(cot, w_out[...], COLS).astype(bf16)
    for h in range(heads):
        a = att[:, h * HD : (h + 1) * HD]
        p = probs[h]
        dp = dot(a, qkv[2 * heads + h], COLS)
        along = jnp.sum(p * dp, axis=-1, keepdims=True)
        ds = (p * (dp - along) * SCALE).astype(bf16)
        for s, got in enumerate(
            (
                dot(ds, qkv[heads + h]),
                dot(ds, qkv[h], ROWS),
                dot(p.astype(bf16), a, ROWS),
            )
        ):
            at = s * narrow + h * HD
            grads[:, at : at + HD] = got.astype(bf16)


def input_back(where, grads, w, own_o, oth_o):
    narrow = w.shape[2]
    part = dot(grads[:, :narrow], w[0], COLS)
    part = part + dot(grads[:, narrow : 2 * narrow], w[1], COLS)
    part = (part + dot(grads[:, 2 * narrow :], w[2], COLS)).astype(bf16)
    for c in range(2):

        @pl.when(where[1] == c)
        def _():
            for half, core in ((own_o, c), (oth_o, 1 - c)):
                for y in range(2):
                    at = (2 * y + core) * narrow
                    half[:, y * narrow : (y + 1) * narrow] = part[:, at : at + narrow]


def first_body(where, t0, ty, tc, tcy, w_out, qkv, probs, w, cot_o, own_o, oth_o, grads):
    put_pieces(where, cot_o, (t0, ty, tc, tcy))
    attention_back(cot_o[...], w_out, qkv, probs, grads)
    input_back(where, grads, w, own_o, oth_o)


def term_of(g, normal, inv):
    width = g.shape[1]
    n = normal[...].astype(f32)
    mean = jnp.sum(g, axis=-1, keepdims=True) * (1.0 / width)
    along = jnp.sum(g * n, axis=-1, keepdims=True) * (1.0 / width)
    return (g - mean - n * along) * inv[:, :1]


def middle_body(where, own, oth, normal, inv, w_out, qkv, probs, w, term_o, own_o, oth_o, spot, grads):
    put_halves(where, spot, own, oth)
    term_o[...] = term_of(spot[...], normal, inv)
    attention_back(term_o[...].astype(bf16), w_out, qkv, probs, grads)
    input_back(where, grads, w, own_o, oth_o)


def last_body(where, own, oth, normal, inv, w_out, qkv, probs, cot, term, mine, imp_o, grads_o, tt_o, spot):
    put_halves(where, spot, own, oth)
    spot[...] = term_of(spot[...], normal, inv) + term[...]
    narrow = mine.shape[1]
    for g in range(4):

        @pl.when(where[0] == g)
        def _():
            imp_o[...] = mine[...] + spot[:, g * narrow : (g + 1) * narrow]

    total = (spot[...] + cot[...].astype(f32)).astype(bf16)
    tt_o[...] = total.T
    attention_back(total, w_out, qkv, probs, grads_o)


def value_rows_body(other, where, xt, tt, grads, att, out):
    narrow = att.shape[1]
    rows = out.shape[1]
    yh = 1 - where[3] if other else where[3]
    for x in range(out.shape[0]):
        at = pl.ds(pl.multiple_of(x * 2 * rows + yh * rows, 16), rows)
        out[x, :, :narrow] = dot(xt[at, :], grads[:, 2 * narrow :]).astype(bf16)
        out[x, :, narrow:] = dot(tt[at, :], att[...]).astype(bf16)


def query_rows_body(steps, where, xt, grads, *outs):
    rows, cols = outs[0].shape
    for step, out in zip(steps, outs):
        at = pl.ds(pl.multiple_of(lax.rem(where[2] + step, 4) * rows, 16), rows)
        out[...] = dot(xt[at, :], grads[:, :cols]).astype(bf16)


def shift(n, by):
    return [(i, (i + by) % n) for i in range(n)]


def add(*parts):
    return sum(p.astype(f32) for p in parts).astype(bf16)


def mp_sum(own, oth):
    chip = add(own, lax.ppermute(oth, "c", SWAP))
    whole = add(chip, lax.ppermute(chip, "yl", SWAP))
    return whole, lax.ppermute(whole, "c", SWAP)


def pieces_of(mine):
    y = lax.ppermute(mine, "yl", SWAP)
    return mine, y, lax.ppermute(mine, "c", SWAP), lax.ppermute(y, "c", SWAP)


def shards(z_star, cotangent, w_qkv, w_out):
    images, tokens, narrow = z_star.shape
    width = 4 * narrow
    heads = narrow // HD
    nx, ny, nz = [lax.axis_size(a) for a in DP]
    x, yh = lax.axis_index("x"), lax.axis_index("yh")
    where = jnp.stack([lax.axis_index(MP), lax.axis_index("c"), x, yh]).astype(jnp.int32)

    z = pieces_of(z_star[0])
    t = pieces_of(cotangent[0].astype(bf16))
    wide = like((tokens, width), bf16)
    half = like((tokens, 2 * narrow), bf16)
    proj = 2 * tokens * width * narrow
    small = 2 * tokens * tokens * HD * heads
    spot = pltpu.VMEM((tokens, width), f32)
    g_like = like((tokens, 3 * narrow), bf16)
    grads_at = pltpu.VMEM((tokens, 3 * narrow), bf16)
    normal, xt, inv, qkv, probs, att = call(
        forward_body,
        (
            wide,
            like((width, tokens), bf16),
            like((tokens, 128), f32),
            like((3 * heads, tokens, HD), bf16),
            like((heads, tokens, tokens), f32),
            like((tokens, narrow), bf16),
        ),
        (where, *z, w_qkv),
        [pltpu.VMEM((tokens, width), bf16)],
        flops=3 * proj + 2 * small,
        name="forward",
    )
    cot, own, oth = call(
        first_body,
        (wide, half, half),
        (where, *t, w_out, qkv, probs, w_qkv),
        [grads_at],
        flops=4 * proj + 4 * small,
        name="first",
    )
    own, oth = mp_sum(own, oth)
    term, own, oth = call(
        middle_body,
        (like((tokens, width), f32), half, half),
        (where, own, oth, normal, inv, w_out, qkv, probs, w_qkv),
        [spot, grads_at],
        flops=4 * proj + 4 * small,
        name="middle",
    )
    own, oth = mp_sum(own, oth)
    implicit, grads, tt = call(
        last_body,
        (like((tokens, narrow), f32), g_like, like((width, tokens), bf16)),
        (where, own, oth, normal, inv, w_out, qkv, probs, cot, term, cotangent[0]),
        [spot],
        flops=proj + 4 * small,
        name="last",
    )

    rows = width // (nx * ny)
    v_like = like((nx, rows, 2 * narrow), bf16)
    q_like = like((ny * rows, 2 * narrow), bf16)
    (v_send,) = call(
        functools.partial(value_rows_body, True),
        (v_like,),
        (where, xt, tt, grads, att),
        flops=proj,
        name="value_send",
    )
    v_got = lax.ppermute(v_send, "yh", SWAP)
    q_send = call(
        functools.partial(query_rows_body, (2, 1, 3)),
        (q_like,) * 3,
        (where, xt, grads),
        flops=2 * proj * 3 // 4,
        name="query_send",
    )
    q_got = [lax.ppermute(s, "x", shift(nx, by)) for s, by in zip(q_send, (2, 1, 3))]
    (v_keep,) = call(
        functools.partial(value_rows_body, False),
        (v_like,),
        (where, xt, tt, grads, att),
        flops=proj,
        name="value_keep",
    )
    (q_keep,) = call(
        functools.partial(query_rows_body, (0,)),
        (q_like,),
        (where, xt, grads),
        flops=2 * proj // 4,
        name="query_keep",
    )
    take = lambda a, j, n: lax.dynamic_index_in_dim(a, lax.rem(j, n), 0, keepdims=False)
    v = add(v_keep, v_got)
    v_got = [lax.ppermute(take(v, x + by, nx), "x", shift(nx, by)) for by in (2, 1, 3)]
    q = add(q_keep, *q_got).reshape(ny, rows, 2 * narrow)
    q_got = lax.ppermute(take(q, yh + 1, ny), "yh", SWAP)
    q = add(take(q, yh, ny), q_got)
    v = add(take(v, x, nx), *v_got)
    both = jnp.concatenate([q, v], axis=1).reshape(nz, rows // nz, width)
    got = lax.all_to_all(both, "z", 0, 0, tiled=True)
    factor = 1.0 / math.sqrt(images * nx * ny * nz * tokens)
    got = jnp.sum(got.astype(f32), axis=0) * factor
    grad_qkv = jnp.stack([got[:, s * narrow : (s + 1) * narrow] for s in range(3)])
    return implicit[None], grad_qkv, got[:, 3 * narrow :].T


def solution(mesh):
    split = Mesh(mesh.devices.reshape(4, 2, 8, 2, 2), AXES)
    return jax.shard_map(
        shards,
        mesh=split,
        in_specs=(P(DP, None, MP), P(DP, None, MP), P(None, None, MP), P(MP, None)),
        out_specs=(P(DP, None, MP), P(None, DP, MP), P(MP, DP)),
        check_vma=False,
    )
```

```python
import functools
import math

import jax
import jax.numpy as jnp
from jax import lax
from jax.experimental import pallas as pl
from jax.experimental.pallas import tpu as pltpu
from jax.sharding import Mesh
from jax.sharding import PartitionSpec as P


HD = 80
AXES = ("x", "yh", "z", "yl", "c")
DP = ("x", "yh", "z")
MP = ("yl", "c")
SWAP = [(0, 1), (1, 0)]

epsilon = 1e-06
f32 = jnp.float32
bf16 = jnp.bfloat16
SCALE = HD ** (-0.5)
ROWS = (((0,), (0,)), ((), ()))
COLS = (((1,), (1,)), ((), ()))


def dot(a, b, dims=(((1,), (0,)), ((), ()))):
    return lax.dot_general(a, b, dims, preferred_element_type=f32)


def call(body, outs, ins, scratch=(), flops=0):
    vmem = pl.BlockSpec(memory_space=pltpu.VMEM)
    smem = pl.BlockSpec(memory_space=pltpu.SMEM)
    size = sum(math.prod(o.shape) * o.dtype.itemsize for o in list(outs) + list(ins))
    return pl.pallas_call(
        body,
        out_shape=outs,
        in_specs=[smem] + [vmem] * (len(ins) - 1),
        out_specs=[vmem] * len(outs),
        scratch_shapes=list(scratch),
        compiler_params=pltpu.CompilerParams(vmem_limit_bytes=28 * 2**20),
        cost_estimate=pl.CostEstimate(flops=flops, bytes_accessed=size, transcendentals=0),
    )(*ins)


def like(shape, dtype):
    return jax.ShapeDtypeStruct(shape, dtype)


def put_pieces(where, spot, pieces):
    narrow = pieces[0].shape[1]
    for g in range(4):

        @pl.when(where[0] == g)
        def _():
            for r, piece in zip((0, 2, 1, 3), pieces):
                at = (g ^ r) * narrow
                spot[:, at : at + narrow] = piece[...].astype(spot.dtype)


def put_halves(where, spot, own, oth):
    narrow = own.shape[1] // 2
    for c in range(2):

        @pl.when(where[1] == c)
        def _():
            for half, core in ((own, c), (oth, 1 - c)):
                for y in range(2):
                    at = (2 * y + core) * narrow
                    spot[:, at : at + narrow] = half[:, y * narrow : (y + 1) * narrow].astype(spot.dtype)


def forward_body(where, z0, zy, zc, zcy, w, normal_o, xt_o, inv_o, qkv_o, probs_o, att_o, zs):
    put_pieces(where, zs, (z0, zy, zc, zcy))
    width = zs.shape[1]
    narrow = w.shape[1]
    values = zs[...].astype(f32)
    centred = values - jnp.sum(values, axis=-1, keepdims=True) * (1.0 / width)
    inv = lax.rsqrt(jnp.sum(centred * centred, axis=-1, keepdims=True) * (1.0 / width) + epsilon)
    inv_o[...] = jnp.broadcast_to(inv, inv_o.shape)
    normal_o[...] = (centred * inv).astype(bf16)
    heads = narrow // HD
    for s in range(3):
        got = dot(normal_o[...], w[s], COLS).astype(bf16)
        for h in range(heads):
            qkv_o[s * heads + h] = got[:, h * HD : (h + 1) * HD]
    for h in range(heads):
        scores = dot(qkv_o[h], qkv_o[heads + h], COLS) * SCALE
        top = jnp.max(scores, axis=-1, keepdims=True)
        e = jnp.exp(scores - top)
        probs = e / jnp.sum(e, axis=-1, keepdims=True)
        probs_o[h] = probs
        att_o[:, h * HD : (h + 1) * HD] = dot(probs.astype(bf16), qkv_o[2 * heads + h]).astype(bf16)
    xt_o[...] = normal_o[...].T


def attention_back(cot, w_out, qkv, probs, grads):
    narrow = w_out.shape[0]
    heads = narrow // HD
    att = dot(cot, w_out[...], COLS).astype(bf16)
    for h in range(heads):
        a = att[:, h * HD : (h + 1) * HD]
        p = probs[h]
        dp = dot(a, qkv[2 * heads + h], COLS)
        along = jnp.sum(p * dp, axis=-1, keepdims=True)
        ds = (p * (dp - along) * SCALE).astype(bf16)
        for s, got in enumerate(
            (
                dot(ds, qkv[heads + h]),
                dot(ds, qkv[h], ROWS),
                dot(p.astype(bf16), a, ROWS),
            )
        ):
            at = s * narrow + h * HD
            grads[:, at : at + HD] = got.astype(bf16)


def input_back(where, grads, w, own_o, oth_o):
    narrow = w.shape[1]
    part = dot(grads[:, :narrow], w[0])
    part = part + dot(grads[:, narrow : 2 * narrow], w[1])
    part = (part + dot(grads[:, 2 * narrow :], w[2])).astype(bf16)
    for c in range(2):

        @pl.when(where[1] == c)
        def _():
            for half, core in ((own_o, c), (oth_o, 1 - c)):
                for y in range(2):
                    at = (2 * y + core) * narrow
                    half[:, y * narrow : (y + 1) * narrow] = part[:, at : at + narrow]


def first_body(where, t0, ty, tc, tcy, w_out, qkv, probs, w, cot_o, own_o, oth_o, grads):
    put_pieces(where, cot_o, (t0, ty, tc, tcy))
    attention_back(cot_o[...], w_out, qkv, probs, grads)
    input_back(where, grads, w, own_o, oth_o)


def term_of(g, normal, inv):
    width = g.shape[1]
    n = normal[...].astype(f32)
    mean = jnp.sum(g, axis=-1, keepdims=True) * (1.0 / width)
    along = jnp.sum(g * n, axis=-1, keepdims=True) * (1.0 / width)
    return (g - mean - n * along) * inv[:, :1]


def middle_body(where, own, oth, normal, inv, w_out, qkv, probs, w, term_o, own_o, oth_o, spot, grads):
    put_halves(where, spot, own, oth)
    term_o[...] = term_of(spot[...], normal, inv)
    attention_back(term_o[...].astype(bf16), w_out, qkv, probs, grads)
    input_back(where, grads, w, own_o, oth_o)


def total_body(where, own, oth, normal, inv, cot, term, mine, att, imp_o, total_o, rows_o, spot):
    put_halves(where, spot, own, oth)
    spot[...] = term_of(spot[...], normal, inv) + term[...]
    narrow = mine.shape[1]
    for g in range(4):

        @pl.when(where[0] == g)
        def _():
            imp_o[...] = mine[...] + spot[:, g * narrow : (g + 1) * narrow]

    total = (spot[...] + cot[...].astype(f32)).astype(bf16)
    total_o[...] = total
    got = dot(total, att[...], ROWS)
    nz, _, _ = rows_o.shape
    each = total.shape[1] // (nz * 8)
    for d in range(8):
        for z in range(nz):
            at = (d * nz + z) * each
            rows_o[z, d * each : (d + 1) * each, :] = got[at : at + each, :].astype(bf16)


def last_body(where, total, w_out, qkv, probs, grads_o):
    attention_back(total[...], w_out, qkv, probs, grads_o)


def value_rows_body(other, first, where, xt, grads, out):
    rows = out.shape[1]
    yh = 1 - where[3] if other else where[3]
    for x in range(out.shape[0]):
        at = pl.ds(pl.multiple_of(x * 2 * rows + yh * rows, 16), rows)
        out[x] = dot(xt[at, :], grads[:, first:]).astype(bf16)


def query_rows_body(steps, where, xt, grads, *outs):
    rows, cols = outs[0].shape
    for step, out in zip(steps, outs):
        at = pl.ds(pl.multiple_of(lax.rem(where[2] + step, 4) * rows, 16), rows)
        out[...] = dot(xt[at, :], grads[:, :cols]).astype(bf16)


def shift(n, by):
    return [(i, (i + by) % n) for i in range(n)]


def add(*parts):
    return sum(p.astype(f32) for p in parts).astype(bf16)


def mp_sum(own, oth):
    chip = add(own, lax.ppermute(oth, "c", SWAP))
    whole = add(chip, lax.ppermute(chip, "yl", SWAP))
    return whole, lax.ppermute(whole, "c", SWAP)


def pieces_of(mine):
    y = lax.ppermute(mine, "yl", SWAP)
    return mine, y, lax.ppermute(mine, "c", SWAP), lax.ppermute(y, "c", SWAP)


def shards(z_star, cotangent, w_qkv, w_out):
    images, tokens, narrow = z_star.shape
    width = 4 * narrow
    heads = narrow // HD
    nx, ny, nz = [lax.axis_size(a) for a in DP]
    x, yh = lax.axis_index("x"), lax.axis_index("yh")
    where = jnp.stack([lax.axis_index(MP), lax.axis_index("c"), x, yh]).astype(jnp.int32)

    w_t = jnp.swapaxes(w_qkv, 1, 2)
    z = pieces_of(z_star[0])
    t = pieces_of(cotangent[0].astype(bf16))
    wide = like((tokens, width), bf16)
    half = like((tokens, 2 * narrow), bf16)
    proj = 2 * tokens * width * narrow
    small = 2 * tokens * tokens * HD * heads
    spot = pltpu.VMEM((tokens, width), f32)
    g_like = like((tokens, 3 * narrow), bf16)
    grads_at = pltpu.VMEM((tokens, 3 * narrow), bf16)
    normal, xt, inv, qkv, probs, att = call(
        forward_body,
        (
            wide,
            like((width, tokens), bf16),
            like((tokens, 128), f32),
            like((3 * heads, tokens, HD), bf16),
            like((heads, tokens, tokens), f32),
            like((tokens, narrow), bf16),
        ),
        (where, *z, w_t),
        [pltpu.VMEM((tokens, width), bf16)],
        flops=3 * proj + 2 * small,
    )
    cot, own, oth = call(
        first_body,
        (wide, half, half),
        (where, *t, w_out, qkv, probs, w_t),
        [grads_at],
        flops=4 * proj + 4 * small,
    )
    own, oth = mp_sum(own, oth)
    term, own, oth = call(
        middle_body,
        (like((tokens, width), f32), half, half),
        (where, own, oth, normal, inv, w_out, qkv, probs, w_t),
        [spot, grads_at],
        flops=4 * proj + 4 * small,
    )
    own, oth = mp_sum(own, oth)
    rows = width // (nx * ny)
    implicit, total, o_rows = call(
        total_body,
        (like((tokens, narrow), f32), wide, like((nz, rows, narrow), bf16)),
        (where, own, oth, normal, inv, cot, term, cotangent[0], att),
        [spot],
        flops=proj,
    )
    o_got = lax.all_to_all(o_rows, "z", 0, 0, tiled=True)
    (grads,) = call(last_body, (g_like,), (where, total, w_out, qkv, probs), flops=proj + 4 * small)

    first = 512
    v_like = like((nx, rows, 3 * narrow - first), bf16)
    q_like = like((ny * rows, first), bf16)
    v_flops = 2 * tokens * (width // 2) * (3 * narrow - first)
    q_flops = 2 * tokens * (width // 4) * first
    (v_send,) = call(
        functools.partial(value_rows_body, True, first),
        (v_like,),
        (where, xt, grads),
        flops=v_flops,
    )
    v_got = lax.ppermute(v_send, "yh", SWAP)
    q_send = call(
        functools.partial(query_rows_body, (2, 1, 3)),
        (q_like,) * 3,
        (where, xt, grads),
        flops=3 * q_flops,
    )
    q_got = [lax.ppermute(s, "x", shift(nx, by)) for s, by in zip(q_send, (2, 1, 3))]
    (v_keep,) = call(
        functools.partial(value_rows_body, False, first),
        (v_like,),
        (where, xt, grads),
        flops=v_flops,
    )
    (q_keep,) = call(
        functools.partial(query_rows_body, (0,)), (q_like,), (where, xt, grads), flops=q_flops
    )
    take = lambda a, j, n: lax.dynamic_index_in_dim(a, lax.rem(j, n), 0, keepdims=False)
    v_got, q_got, o_got = lax.optimization_barrier((v_got, q_got, o_got))
    v = add(v_keep, v_got)
    v_got = [lax.ppermute(take(v, x + by, nx), "x", shift(nx, by)) for by in (2, 1, 3)]
    q = add(q_keep, *q_got).reshape(ny, rows, first)
    q_got = lax.ppermute(take(q, yh + 1, ny), "yh", SWAP)
    o = jnp.sum(o_got.astype(f32), axis=0).astype(bf16).reshape(nx * ny, rows // nz, narrow)
    o = lax.all_to_all(o, ("x", "yh"), 0, 0, tiled=True)
    q_got, v_got, o = lax.optimization_barrier((q_got, v_got, o))
    q = add(take(q, yh, ny), q_got)
    v = add(take(v, x, nx), *v_got)
    both = jnp.concatenate([q, v], axis=1).reshape(nz, rows // nz, 3 * narrow)
    got = lax.all_to_all(both, "z", 0, 0, tiled=True)
    factor = 1.0 / math.sqrt(images * nx * ny * nz * tokens)
    got = jnp.sum(got.astype(f32), axis=0) * factor
    o = jnp.sum(o.astype(f32), axis=0) * factor
    grad_qkv = jnp.stack([got[:, s * narrow : (s + 1) * narrow] for s in range(3)])
    return implicit[None], grad_qkv, o.T


def solution(mesh):
    split = Mesh(mesh.devices.reshape(4, 2, 8, 2, 2), AXES)


    return jax.shard_map(
        shards,
        mesh=split,
        in_specs=(P(DP, None, MP), P(DP, None, MP), P(None, None, MP), P(MP, None)),
        out_specs=(P(DP, None, MP), P(None, DP, MP), P(MP, DP)),
        check_vma=False,
    )
```

```python
import functools
import math

import jax
import jax.numpy as jnp
from jax import lax
from jax.experimental import pallas as pl
from jax.experimental.pallas import tpu as pltpu
from jax.sharding import Mesh
from jax.sharding import PartitionSpec as P


HD = 80
AXES = ("x", "yh", "z", "yl", "c")
DP = ("x", "yh", "z")
MP = ("yl", "c")
SWAP = [(0, 1), (1, 0)]
MINE, OTHER = 0, 1

epsilon = 1e-06
f32 = jnp.float32
bf16 = jnp.bfloat16
SCALE = HD ** (-0.5)
ROWS = (((0,), (0,)), ((), ()))
COLS = (((1,), (1,)), ((), ()))


def dot(a, b, dims=(((1,), (0,)), ((), ()))):
    return lax.dot_general(a, b, dims, preferred_element_type=f32)


def call(body, outs, ins, scratch=(), flops=0):
    vmem = pl.BlockSpec(memory_space=pltpu.VMEM)
    smem = pl.BlockSpec(memory_space=pltpu.SMEM)
    size = sum(math.prod(o.shape) * o.dtype.itemsize for o in list(outs) + list(ins))
    return pl.pallas_call(
        body,
        out_shape=outs,
        in_specs=[smem] + [vmem] * (len(ins) - 1),
        out_specs=[vmem] * len(outs),
        scratch_shapes=list(scratch),
        compiler_params=pltpu.CompilerParams(vmem_limit_bytes=20 * 2**20),
        cost_estimate=pl.CostEstimate(flops=flops, bytes_accessed=size, transcendentals=0),
    )(*ins)


def like(shape, dtype):
    return jax.ShapeDtypeStruct(shape, dtype)


def prepare_body(where, cot, w, w_out, cot_o, w_o, w_out_o):
    narrow = w_out.shape[0]
    cot_o[...] = cot[...].astype(bf16)
    for c in range(2):

        @pl.when(where[1] == c)
        def _():
            for k, core in enumerate((c, 1 - c)):
                for y in range(2):
                    src = (2 * y + core) * narrow
                    at = (2 * k + y) * narrow
                    w_out_o[:, at : at + narrow] = w_out[:, src : src + narrow]
                    for s in range(3):
                        w_o[s * narrow : (s + 1) * narrow, at : at + narrow] = w[s, :, src : src + narrow]


def put_pieces(where, spot, mine, y, core, both):
    narrow = mine.shape[1]
    for yl in range(2):

        @pl.when(where[0] == yl)
        def _():
            for k, (near, far) in enumerate(((mine, y), (core, both))):
                for at, piece in ((2 * k + yl, near), (2 * k + 1 - yl, far)):
                    spot[:, at * narrow : (at + 1) * narrow] = piece[...]


def forward_body(where, z0, zy, zc, zcy, w, normal_o, xt_o, inv_o, qkv_o, probs_o, att_o, zs):
    put_pieces(where, zs, z0, zy, zc, zcy)
    width = zs.shape[1]
    narrow = width // 4
    values = zs[...].astype(f32)
    centred = values - jnp.sum(values, axis=-1, keepdims=True) * (1.0 / width)
    inv = lax.rsqrt(jnp.sum(centred * centred, axis=-1, keepdims=True) * (1.0 / width) + epsilon)
    inv_o[...] = jnp.broadcast_to(inv, inv_o.shape)
    normal_o[...] = (centred * inv).astype(bf16)
    heads = narrow // HD
    for s in range(3):
        got = dot(normal_o[...], w[s * narrow : (s + 1) * narrow, :], COLS).astype(bf16)
        for h in range(heads):
            qkv_o[s * heads + h] = got[:, h * HD : (h + 1) * HD]
    for h in range(heads):
        scores = dot(qkv_o[h], qkv_o[heads + h], COLS) * SCALE
        top = jnp.max(scores, axis=-1, keepdims=True)
        e = jnp.exp(scores - top)
        probs = e / jnp.sum(e, axis=-1, keepdims=True)
        probs_o[h] = probs
        att_o[:, h * HD : (h + 1) * HD] = dot(probs.astype(bf16), qkv_o[2 * heads + h]).astype(bf16)
    xt_o[...] = normal_o[...].T


def attention_back(cot, w_out, qkv, probs, grads):
    narrow = w_out.shape[0]
    heads = narrow // HD
    att = dot(cot, w_out[...], COLS).astype(bf16)
    for h in range(heads):
        a = att[:, h * HD : (h + 1) * HD]
        p = probs[h]
        dp = dot(a, qkv[2 * heads + h], COLS)
        along = jnp.sum(p * dp, axis=-1, keepdims=True)
        ds = (p * (dp - along) * SCALE).astype(bf16)
        for s, got in enumerate(
            (
                dot(ds, qkv[heads + h]),
                dot(ds, qkv[h], ROWS),
                dot(p.astype(bf16), a, ROWS),
            )
        ):
            at = s * narrow + h * HD
            grads[:, at : at + HD] = got.astype(bf16)


def input_back(half, grads, w):
    wide = w.shape[1] // 2
    return dot(grads[...], w[:, half * wide : (half + 1) * wide]).astype(bf16)


def first_body(where, t0, ty, tc, tcy, w_out, qkv, probs, w, cot_o, grads_o, oth_o):
    put_pieces(where, cot_o, t0, ty, tc, tcy)
    attention_back(cot_o[...], w_out, qkv, probs, grads_o)
    oth_o[...] = input_back(OTHER, grads_o, w)


def own_body(where, grads, w, own_o):
    own_o[...] = input_back(MINE, grads, w)


def put_term(spot, chip, far, chip_c, far_c, normal, inv):
    half = chip.shape[1]
    spot[:, :half] = chip[...].astype(f32) + far[...].astype(f32)
    spot[:, half:] = chip_c[...].astype(f32) + far_c[...].astype(f32)
    g = spot[...]
    width = g.shape[1]
    n = normal[...].astype(f32)
    mean = jnp.sum(g, axis=-1, keepdims=True) * (1.0 / width)
    along = jnp.sum(g * n, axis=-1, keepdims=True) * (1.0 / width)
    return (g - mean - n * along) * inv[:, :1]


def middle_body(where, chip, far, chip_c, far_c, normal, inv, w_out, qkv, probs, w, term_o, grads_o, oth_o):
    term_o[...] = put_term(term_o, chip, far, chip_c, far_c, normal, inv)
    attention_back(term_o[...].astype(bf16), w_out, qkv, probs, grads_o)
    oth_o[...] = input_back(OTHER, grads_o, w)


def last_body(where, chip, far, chip_c, far_c, normal, inv, w_out, qkv, probs, cot, term, mine, imp_o, grads_o, total_o, spot):
    spot[...] = put_term(spot, chip, far, chip_c, far_c, normal, inv) + term[...]
    narrow = mine.shape[1]
    for yl in range(2):

        @pl.when(where[0] == yl)
        def _():
            imp_o[...] = mine[...] + spot[:, yl * narrow : (yl + 1) * narrow]

    total = (spot[...] + cot[...].astype(f32)).astype(bf16)
    total_o[...] = total
    attention_back(total, w_out, qkv, probs, grads_o)


def spot_of(where, x, narrow):
    other = lax.rem(x + where[1], 2)
    return (2 * other + lax.div(x, 2)) * narrow


def gather_rows(where, src, dst, picks, narrow):
    rows = narrow // 2
    for i, (dx, dy) in enumerate(picks):
        at = spot_of(where, lax.bitwise_xor(where[2], dx), narrow)
        at = at + lax.bitwise_xor(where[3], dy) * rows
        dst[i * rows : (i + 1) * rows, :] = src[pl.ds(pl.multiple_of(at, 16), rows), :]


def rows_body(picks, first, where, xt, grads, out, xs):
    gather_rows(where, xt, xs, picks, grads.shape[1] // 3)
    out[...] = dot(xs[...], grads[:, first : first + out.shape[1]]).astype(bf16)


def turn_body(where, total, tt_o):
    tt_o[...] = total[...].T


def tail_rows_body(picks, where, xt, tt, grads, att, out, xs):
    narrow = att.shape[1]
    left = out.shape[1] - narrow
    gather_rows(where, xt, xs, picks, narrow)
    one = dot(xs[...], grads[:, grads.shape[1] - left :])
    gather_rows(where, tt, xs, picks, narrow)
    two = dot(xs[...], att[...])
    out[:, :left] = one.astype(bf16)
    out[:, left:] = two.astype(bf16)


def pack_body(where, k1, g1, k2, g2, k3, g3, out, spot):
    at = 0
    for k, g in ((k1, g1), (k2, g2), (k3, g3)):
        spot[:, at : at + k.shape[1]] = k[...].astype(f32) + g[...].astype(f32)
        at += k.shape[1]
    nz, _, lanes = out.shape
    each = spot.shape[0] // nz
    for z in range(nz):
        for b in range(spot.shape[1] // lanes):
            piece = spot[z * each : (z + 1) * each, b * lanes : (b + 1) * lanes]
            out[z, b * each : (b + 1) * each, :] = piece.astype(bf16)


def unpack_body(factor, where, got, qkv_o, out_o, spot):
    total = got[0].astype(f32)
    for z in range(1, got.shape[0]):
        total = total + got[z].astype(f32)
    total = total * factor
    each, width = spot.shape
    lanes = got.shape[2]
    for b in range(width // lanes):
        spot[:, b * lanes : (b + 1) * lanes] = total[b * each : (b + 1) * each, :]
    narrow = out_o.shape[1]
    for k in range(3):
        qkv_o[k] = spot[:, k * narrow : (k + 1) * narrow]
    out_o[...] = spot[:, 3 * narrow :]


def add(*parts):
    return sum(p.astype(f32) for p in parts).astype(bf16)


def mp_sum(oth, own):
    chip = add(own(), lax.ppermute(oth, "c", SWAP))
    far = lax.ppermute(chip, "yl", SWAP)
    return chip, far, lax.ppermute(chip, "c", SWAP), lax.ppermute(far, "c", SWAP)


def shards(z_star, cotangent, w_qkv, w_out):
    images, tokens, narrow = z_star.shape
    width = 4 * narrow
    heads = narrow // HD
    nx, ny, nz = [lax.axis_size(a) for a in DP]
    x, yh = lax.axis_index("x"), lax.axis_index("yh")
    where = jnp.stack([lax.axis_index("yl"), lax.axis_index("c"), x, yh]).astype(jnp.int32)

    wide = like((tokens, width), bf16)
    wide_f = like((tokens, width), f32)
    half = like((tokens, 2 * narrow), bf16)
    g_like = like((tokens, 3 * narrow), bf16)
    proj = 2 * tokens * width * narrow
    small = 2 * tokens * tokens * HD * heads

    z0 = z_star[0]
    zy = lax.ppermute(z0, "yl", SWAP)
    zc = lax.ppermute(z0, "c", SWAP)
    t0, w, wo = call(
        prepare_body,
        (like((tokens, narrow), bf16), like((3 * narrow, width), bf16), like((narrow, width), bf16)),
        (where, cotangent[0], jnp.swapaxes(w_qkv, 1, 2), w_out),
        flops=proj,
    )
    tc = lax.ppermute(t0, "c", SWAP)
    zy, t0 = lax.optimization_barrier((zy, t0))
    zcy = lax.ppermute(zy, "c", SWAP)
    ty = lax.ppermute(t0, "yl", SWAP)
    tcy = lax.ppermute(ty, "c", SWAP)
    normal, xt, inv, qkv, probs, att = call(
        forward_body,
        (
            wide,
            like((width, tokens), bf16),
            like((tokens, 128), f32),
            like((3 * heads, tokens, HD), bf16),
            like((heads, tokens, tokens), f32),
            like((tokens, narrow), bf16),
        ),
        (where, z0, zy, zc, zcy, w),
        [pltpu.VMEM((tokens, width), bf16)],
        flops=3 * proj + 2 * small,
    )

    def own_of(grads):
        return call(own_body, (half,), (where, grads, w), flops=3 * proj // 2)[0]

    cot, grads, oth = call(
        first_body,
        (wide, g_like, half),
        (where, t0, ty, tc, tcy, wo, qkv, probs, w),
        flops=3 * proj + 4 * small,
    )
    sums = mp_sum(oth, lambda: own_of(grads))
    term, grads, oth = call(
        middle_body,
        (wide_f, g_like, half),
        (where, *sums, normal, inv, wo, qkv, probs, w),
        flops=3 * proj + 4 * small,
    )
    sums = mp_sum(oth, lambda: own_of(grads))
    implicit, grads, total = call(
        last_body,
        (like((tokens, narrow), f32), g_like, wide),
        (where, *sums, normal, inv, wo, qkv, probs, cot, term, cotangent[0]),
        [pltpu.VMEM((tokens, width), f32)],
        flops=proj + 4 * small,
    )

    rows = width // (nx * ny)
    each = rows // nz
    tall = [pltpu.VMEM((4 * rows, tokens), bf16)]

    def block(picks, first, cols):
        return call(
            functools.partial(rows_body, picks, first),
            (like((4 * rows, cols), bf16),),
            (where, xt, grads),
            tall,
            flops=2 * tokens * 4 * rows * cols,
        )[0]

    def tail_block(picks, cols):
        return call(
            functools.partial(tail_rows_body, picks),
            (like((4 * rows, cols), bf16),),
            (where, xt, tt, grads, att),
            tall,
            flops=2 * tokens * 4 * rows * cols,
        )[0]

    def swap_x(value, by):
        return lax.ppermute(value, "x", [(i, i ^ by) for i in range(nx)])

    def swap_yh(value):
        return lax.ppermute(value, "yh", SWAP)

    def at(value, start, count):
        return value[start * rows : (start + count) * rows]

    one, two, three = 384, 512, 384
    s2 = block(((3, 0), (2, 0), (3, 1), (2, 1)), one, two)
    g2 = swap_x(s2, 3)
    s1 = block(((1, 0), (1, 1), (2, 0), (2, 1)), 0, one)
    g1 = swap_x(s1, 1)
    (tt,) = call(turn_body, (like((width, tokens), bf16),), (where, total), flops=proj)
    s3 = tail_block(((0, 1), (3, 1), (1, 1), (2, 1)), three)
    g3 = swap_yh(s3)
    k2 = block(((0, 0), (1, 0), (0, 1), (1, 1)), one, two)
    k1 = block(((0, 0), (0, 1), (3, 0), (3, 1)), 0, one)
    k3 = tail_block(((0, 0), (3, 0), (1, 0), (2, 0)), three)

    h2 = swap_yh(add(at(k2, 2, 2), at(g2, 2, 2)))
    h1 = swap_x(add(at(k1, 2, 2), at(g1, 2, 2)), 3)
    h3 = swap_x(add(at(k3, 2, 2), at(g3, 2, 2)), 1)

    def last_half(k, g, h, swap):
        send = add(at(k, 1, 1), at(g, 1, 1), at(h, 1, 1))
        got = swap(send)
        return add(at(k, 0, 1), at(g, 0, 1), at(h, 0, 1)), got

    e2 = last_half(k2, g2, h2, lambda v: swap_x(v, 1))
    e1 = last_half(k1, g1, h1, swap_yh)
    e3 = last_half(k3, g3, h3, lambda v: swap_x(v, 3))
    dense = each * width // 128
    (packed,) = call(
        pack_body,
        (like((nz, dense, 128), bf16),),
        (where, *e1, *e2, *e3),
        [pltpu.VMEM((rows, width), f32)],
        flops=rows * width,
    )
    got = lax.all_to_all(packed, "z", 0, 0, tiled=True)
    factor = 1.0 / math.sqrt(images * nx * ny * nz * tokens)
    grad_qkv, grad_o = call(
        functools.partial(unpack_body, factor),
        (like((3, each, narrow), f32), like((each, narrow), f32)),
        (where, got),
        [pltpu.VMEM((each, width), f32)],
        flops=rows * width,
    )
    return implicit[None], grad_qkv, grad_o.T


def solution(mesh):
    split = Mesh(mesh.devices.reshape(4, 2, 8, 2, 2), AXES)

    return jax.shard_map(
        shards,
        mesh=split,
        in_specs=(P(DP, None, MP), P(DP, None, MP), P(None, None, MP), P(MP, None)),
        out_specs=(P(DP, None, MP), P(None, DP, MP), P(MP, DP)),
        check_vma=False,
    )
```

```python
import functools
import math

import jax
import jax.numpy as jnp
from jax import lax
from jax.experimental import pallas as pl
from jax.experimental.pallas import tpu as pltpu
from jax.sharding import Mesh
from jax.sharding import PartitionSpec as P


HD = 80
AXES = ("x", "yh", "z", "yl", "c")
DP = ("x", "yh", "z")
MP = ("yl", "c")
SWAP = [(0, 1), (1, 0)]
MINE, OTHER = 0, 1

epsilon = 1e-06
f32 = jnp.float32
bf16 = jnp.bfloat16
SCALE = HD ** (-0.5)
ROWS = (((0,), (0,)), ((), ()))
COLS = (((1,), (1,)), ((), ()))


def dot(a, b, dims=(((1,), (0,)), ((), ()))):
    return lax.dot_general(a, b, dims, preferred_element_type=f32)


def call(body, outs, ins, scratch=(), flops=0):
    vmem = pl.BlockSpec(memory_space=pltpu.VMEM)
    size = sum(math.prod(o.shape) * o.dtype.itemsize for o in list(outs) + list(ins))
    return pl.pallas_call(
        body,
        out_shape=outs,
        in_specs=[vmem] * len(ins),
        out_specs=[vmem] * len(outs),
        scratch_shapes=list(scratch),
        compiler_params=pltpu.CompilerParams(vmem_limit_bytes=20 * 2**20),
        cost_estimate=pl.CostEstimate(flops=flops, bytes_accessed=size, transcendentals=0),
    )(*ins)


def like(shape, dtype):
    return jax.ShapeDtypeStruct(shape, dtype)


def reordered(dst, rows, src, narrow):
    for c in range(2):

        @pl.when(lax.axis_index("c") == c)
        def _():
            for k, core in enumerate((c, 1 - c)):
                for y in range(2):
                    old = (2 * y + core) * narrow
                    new = (2 * k + y) * narrow
                    dst[rows, new : new + narrow] = src[:, old : old + narrow]


def prepare_body(cot, w, cot_o, w_o):
    narrow = cot.shape[1]
    cot_o[...] = cot[...].astype(bf16)
    for s in range(3):
        reordered(w_o, slice(s * narrow, (s + 1) * narrow), w.at[s], narrow)


def prepare_out_body(w_out, w_out_o):
    reordered(w_out_o, slice(None), w_out, w_out.shape[0])


def put_pieces(spot, mine, y, core, both):
    narrow = mine.shape[1]
    for yl in range(2):

        @pl.when(lax.axis_index("yl") == yl)
        def _():
            for k, (near, far) in enumerate(((mine, y), (core, both))):
                for at, piece in ((2 * k + yl, near), (2 * k + 1 - yl, far)):
                    spot[:, at * narrow : (at + 1) * narrow] = piece[...]


def forward_body(z0, zy, zc, zcy, w, normal_o, xt_o, inv_o, qkv_o, probs_o, att_o, zs):
    put_pieces(zs, z0, zy, zc, zcy)
    width = zs.shape[1]
    narrow = width // 4
    values = zs[...].astype(f32)
    centred = values - jnp.sum(values, axis=-1, keepdims=True) * (1.0 / width)
    inv = lax.rsqrt(jnp.sum(centred * centred, axis=-1, keepdims=True) * (1.0 / width) + epsilon)
    inv_o[...] = jnp.broadcast_to(inv, inv_o.shape)
    normal_o[...] = (centred * inv).astype(bf16)
    heads = narrow // HD
    for s in range(3):
        got = dot(normal_o[...], w[s * narrow : (s + 1) * narrow, :], COLS).astype(bf16)
        for h in range(heads):
            qkv_o[s * heads + h] = got[:, h * HD : (h + 1) * HD]
    xt_o[...] = normal_o[...].T
    scores = [dot(qkv_o[h], qkv_o[heads + h], COLS) * SCALE for h in range(heads)]
    for h in range(heads):
        e = jnp.exp(scores[h] - jnp.max(scores[h], axis=-1, keepdims=True))
        probs_o[h] = e / jnp.sum(e, axis=-1, keepdims=True)
    for h in range(heads):
        att_o[:, h * HD : (h + 1) * HD] = dot(probs_o[h].astype(bf16), qkv_o[2 * heads + h]).astype(bf16)


def attention_back(cot, w_out, qkv, probs, grads):
    narrow = w_out.shape[0]
    heads = narrow // HD
    att = dot(cot, w_out[...], COLS).astype(bf16)
    each = [att[:, h * HD : (h + 1) * HD] for h in range(heads)]

    def put(s, h, got):
        at = s * narrow + h * HD
        grads[:, at : at + HD] = got.astype(bf16)

    dps = [dot(each[h], qkv[2 * heads + h], COLS) for h in range(heads)]
    for h in range(heads):
        put(2, h, dot(probs[h].astype(bf16), each[h], ROWS))
    for h in range(heads):
        p = probs[h]
        along = jnp.sum(p * dps[h], axis=-1, keepdims=True)
        ds = (p * (dps[h] - along) * SCALE).astype(bf16)
        put(0, h, dot(ds, qkv[heads + h]))
        put(1, h, dot(ds, qkv[h], ROWS))


def input_back(half, grads, w):
    wide = w.shape[1] // 2
    return dot(grads[...], w[:, half * wide : (half + 1) * wide]).astype(bf16)


def first_body(t0, ty, tc, tcy, w_out, qkv, probs, w, cot_o, grads_o, oth_o):
    put_pieces(cot_o, t0, ty, tc, tcy)
    attention_back(cot_o[...], w_out, qkv, probs, grads_o)
    oth_o[...] = input_back(OTHER, grads_o, w)


def own_body(grads, w, own_o):
    own_o[...] = input_back(MINE, grads, w)


def put_term(spot, chip, far, chip_c, far_c, normal, inv):
    half = chip.shape[1]
    spot[:, :half] = chip[...].astype(f32) + far[...].astype(f32)
    spot[:, half:] = chip_c[...].astype(f32) + far_c[...].astype(f32)
    g = spot[...]
    width = g.shape[1]
    n = normal[...].astype(f32)
    mean = jnp.sum(g, axis=-1, keepdims=True) * (1.0 / width)
    along = jnp.sum(g * n, axis=-1, keepdims=True) * (1.0 / width)
    return (g - mean - n * along) * inv[:, :1]


def middle_body(chip, far, chip_c, far_c, normal, inv, w_out, qkv, probs, w, term_o, grads_o, oth_o):
    term_o[...] = put_term(term_o, chip, far, chip_c, far_c, normal, inv)
    attention_back(term_o[...].astype(bf16), w_out, qkv, probs, grads_o)
    oth_o[...] = input_back(OTHER, grads_o, w)


def last_body(chip, far, chip_c, far_c, normal, inv, w_out, qkv, probs, cot, term, mine, imp_o, grads_o, total_o, spot):
    spot[...] = put_term(spot, chip, far, chip_c, far_c, normal, inv) + term[...]
    narrow = mine.shape[1]
    for yl in range(2):

        @pl.when(lax.axis_index("yl") == yl)
        def _():
            imp_o[...] = mine[...] + spot[:, yl * narrow : (yl + 1) * narrow]

    total = (spot[...] + cot[...].astype(f32)).astype(bf16)
    total_o[...] = total
    attention_back(total, w_out, qkv, probs, grads_o)


def spot_of(x, narrow):
    other = lax.rem(x + lax.axis_index("c"), 2)
    return (2 * other + lax.div(x, 2)) * narrow


def gather_rows(src, dst, picks, narrow):
    rows = narrow // 2
    for i, (dx, dy) in enumerate(picks):
        at = spot_of(lax.bitwise_xor(lax.axis_index("x"), dx), narrow)
        at = at + lax.bitwise_xor(lax.axis_index("yh"), dy) * rows
        dst[i * rows : (i + 1) * rows, :] = src[pl.ds(pl.multiple_of(at, 16), rows), :]


def rows_body(picks, first, xt, grads, out, xs):
    gather_rows(xt, xs, picks, grads.shape[1] // 3)
    out[...] = dot(xs[...], grads[:, first : first + out.shape[1]]).astype(bf16)


def turn_body(total, tt_o):
    tt_o[...] = total[...].T


def tail_rows_body(picks, xt, tt, grads, att, out, xs):
    narrow = att.shape[1]
    left = out.shape[1] - narrow
    gather_rows(xt, xs, picks, narrow)
    one = dot(xs[...], grads[:, grads.shape[1] - left :])
    gather_rows(tt, xs, picks, narrow)
    two = dot(xs[...], att[...])
    out[:, :left] = one.astype(bf16)
    out[:, left:] = two.astype(bf16)


def pack_body(k1, g1, k2, g2, k3, g3, out, spot):
    at = 0
    for k, g in ((k1, g1), (k2, g2), (k3, g3)):
        spot[:, at : at + k.shape[1]] = k[...].astype(f32) + g[...].astype(f32)
        at += k.shape[1]
    nz, _, lanes = out.shape
    each = spot.shape[0] // nz
    for z in range(nz):
        for b in range(spot.shape[1] // lanes):
            piece = spot[z * each : (z + 1) * each, b * lanes : (b + 1) * lanes]
            out[z, b * each : (b + 1) * each, :] = piece.astype(bf16)


def unpack_body(factor, got, qkv_o, out_o, spot):
    total = got[0].astype(f32)
    for z in range(1, got.shape[0]):
        total = total + got[z].astype(f32)
    total = total * factor
    each, width = spot.shape
    lanes = got.shape[2]
    for b in range(width // lanes):
        spot[:, b * lanes : (b + 1) * lanes] = total[b * each : (b + 1) * each, :]
    narrow = out_o.shape[1]
    for k in range(3):
        qkv_o[k] = spot[:, k * narrow : (k + 1) * narrow]
    out_o[...] = spot[:, 3 * narrow :]


def add(*parts):
    return sum(p.astype(f32) for p in parts).astype(bf16)


def mp_sum(oth, own):
    chip = add(own(), lax.ppermute(oth, "c", SWAP))
    far = lax.ppermute(chip, "yl", SWAP)
    return chip, far, lax.ppermute(chip, "c", SWAP), lax.ppermute(far, "c", SWAP)


def shards(z_star, cotangent, w_qkv, w_out):
    images, tokens, narrow = z_star.shape
    width = 4 * narrow
    heads = narrow // HD
    nx, ny, nz = [lax.axis_size(a) for a in DP]

    wide = like((tokens, width), bf16)
    wide_f = like((tokens, width), f32)
    half = like((tokens, 2 * narrow), bf16)
    g_like = like((tokens, 3 * narrow), bf16)
    proj = 2 * tokens * width * narrow
    small = 2 * tokens * tokens * HD * heads

    z0 = z_star[0]
    zy = lax.ppermute(z0, "yl", SWAP)
    zc = lax.ppermute(z0, "c", SWAP)
    t0, w = call(
        prepare_body,
        (like((tokens, narrow), bf16), like((3 * narrow, width), bf16)),
        (cotangent[0], jnp.swapaxes(w_qkv, 1, 2)),
        flops=proj,
    )
    (wo,) = call(prepare_out_body, (like((narrow, width), bf16),), (w_out,), flops=proj)
    tc = lax.ppermute(t0, "c", SWAP)
    zcy = lax.ppermute(zy, "c", SWAP)
    ty = lax.ppermute(t0, "yl", SWAP)
    tcy = lax.ppermute(ty, "c", SWAP)
    normal, xt, inv, qkv, probs, att = call(
        forward_body,
        (
            wide,
            like((width, tokens), bf16),
            like((tokens, 128), f32),
            like((3 * heads, tokens, HD), bf16),
            like((heads, tokens, tokens), f32),
            like((tokens, narrow), bf16),
        ),
        (z0, zy, zc, zcy, w),
        [pltpu.VMEM((tokens, width), bf16)],
        flops=3 * proj + 2 * small,
    )

    def own_of(grads):
        return call(own_body, (half,), (grads, w), flops=3 * proj // 2)[0]

    cot, grads, oth = call(
        first_body,
        (wide, g_like, half),
        (t0, ty, tc, tcy, wo, qkv, probs, w),
        flops=3 * proj + 4 * small,
    )
    sums = mp_sum(oth, lambda: own_of(grads))
    term, grads, oth = call(
        middle_body,
        (wide_f, g_like, half),
        (*sums, normal, inv, wo, qkv, probs, w),
        flops=3 * proj + 4 * small,
    )
    sums = mp_sum(oth, lambda: own_of(grads))
    implicit, grads, total = call(
        last_body,
        (like((tokens, narrow), f32), g_like, wide),
        (*sums, normal, inv, wo, qkv, probs, cot, term, cotangent[0]),
        [pltpu.VMEM((tokens, width), f32)],
        flops=proj + 4 * small,
    )

    rows = width // (nx * ny)
    each = rows // nz
    tall = [pltpu.VMEM((4 * rows, tokens), bf16)]

    def block(picks, first, cols):
        return call(
            functools.partial(rows_body, picks, first),
            (like((4 * rows, cols), bf16),),
            (xt, grads),
            tall,
            flops=2 * tokens * 4 * rows * cols,
        )[0]

    def tail_block(picks, cols):
        return call(
            functools.partial(tail_rows_body, picks),
            (like((4 * rows, cols), bf16),),
            (xt, tt, grads, att),
            tall,
            flops=2 * tokens * 4 * rows * cols,
        )[0]

    def swap_x(value, by):
        return lax.ppermute(value, "x", [(i, i ^ by) for i in range(nx)])

    def swap_yh(value):
        return lax.ppermute(value, "yh", SWAP)

    def at(value, start, count):
        return value[start * rows : (start + count) * rows]

    one, two, three = 384, 512, 384
    s2 = block(((3, 0), (2, 0), (3, 1), (2, 1)), one, two)
    g2 = swap_x(s2, 3)
    s1 = block(((1, 0), (1, 1), (2, 0), (2, 1)), 0, one)
    g1 = swap_x(s1, 1)
    (tt,) = call(turn_body, (like((width, tokens), bf16),), (total,), flops=proj)
    s3 = tail_block(((0, 1), (3, 1), (1, 1), (2, 1)), three)
    g3 = swap_yh(s3)
    k2 = block(((0, 0), (1, 0), (0, 1), (1, 1)), one, two)
    k1 = block(((0, 0), (0, 1), (3, 0), (3, 1)), 0, one)
    k3 = tail_block(((0, 0), (3, 0), (1, 0), (2, 0)), three)

    h2 = swap_yh(add(at(k2, 2, 2), at(g2, 2, 2)))
    h1 = swap_x(add(at(k1, 2, 2), at(g1, 2, 2)), 3)
    h3 = swap_x(add(at(k3, 2, 2), at(g3, 2, 2)), 1)

    def last_half(k, g, h, swap):
        send = add(at(k, 1, 1), at(g, 1, 1), at(h, 1, 1))
        got = swap(send)
        return add(at(k, 0, 1), at(g, 0, 1), at(h, 0, 1)), got

    e2 = last_half(k2, g2, h2, lambda v: swap_x(v, 1))
    e1 = last_half(k1, g1, h1, swap_yh)
    e3 = last_half(k3, g3, h3, lambda v: swap_x(v, 3))
    dense = each * width // 128
    (packed,) = call(
        pack_body,
        (like((nz, dense, 128), bf16),),
        (*e1, *e2, *e3),
        [pltpu.VMEM((rows, width), f32)],
        flops=rows * width,
    )
    got = lax.all_to_all(packed, "z", 0, 0, tiled=True)
    factor = 1.0 / math.sqrt(images * nx * ny * nz * tokens)
    grad_qkv, grad_o = call(
        functools.partial(unpack_body, factor),
        (like((3, each, narrow), f32), like((each, narrow), f32)),
        (got,),
        [pltpu.VMEM((each, width), f32)],
        flops=rows * width,
    )
    return implicit[None], grad_qkv, grad_o.T


def solution(mesh):
    split = Mesh(mesh.devices.reshape(4, 2, 8, 2, 2), AXES)

    return jax.shard_map(
        shards,
        mesh=split,
        in_specs=(P(DP, None, MP), P(DP, None, MP), P(None, None, MP), P(MP, None)),
        out_specs=(P(DP, None, MP), P(None, DP, MP), P(MP, DP)),
        check_vma=False,
    )
```

```python
import functools
import math

import jax
import jax.numpy as jnp
from jax import lax
from jax.experimental import pallas as pl
from jax.experimental.pallas import tpu as pltpu
from jax.sharding import Mesh
from jax.sharding import PartitionSpec as P


HD = 80
AXES = ("x", "yh", "z", "yl", "c")
DP = ("x", "yh", "z")
MP = ("yl", "c")
SWAP = [(0, 1), (1, 0)]
MINE, OTHER = 0, 1

epsilon = 1e-06
f32 = jnp.float32
bf16 = jnp.bfloat16
SCALE = HD ** (-0.5)
ROWS = (((0,), (0,)), ((), ()))
COLS = (((1,), (1,)), ((), ()))


def dot(a, b, dims=(((1,), (0,)), ((), ()))):
    return lax.dot_general(a, b, dims, preferred_element_type=f32)


def call(body, outs, ins, scratch=(), flops=0):
    vmem = pl.BlockSpec(memory_space=pltpu.VMEM)
    size = sum(math.prod(o.shape) * o.dtype.itemsize for o in list(outs) + list(ins))
    return pl.pallas_call(
        body,
        out_shape=outs,
        in_specs=[vmem] * len(ins),
        out_specs=[vmem] * len(outs),
        scratch_shapes=list(scratch),
        compiler_params=pltpu.CompilerParams(vmem_limit_bytes=20 * 2**20),
        cost_estimate=pl.CostEstimate(flops=flops, bytes_accessed=size, transcendentals=0),
    )(*ins)


def like(shape, dtype):
    return jax.ShapeDtypeStruct(shape, dtype)


def reordered(dst, rows, src, narrow):
    for c in range(2):

        @pl.when(lax.axis_index("c") == c)
        def _():
            for k, core in enumerate((c, 1 - c)):
                for y in range(2):
                    old = (2 * y + core) * narrow
                    new = (2 * k + y) * narrow
                    dst[rows, new : new + narrow] = src[:, old : old + narrow]


def prepare_body(cot, w, cot_o, w_o):
    narrow = cot.shape[1]
    cot_o[...] = cot[...].astype(bf16)
    for s in range(3):
        reordered(w_o, slice(s * narrow, (s + 1) * narrow), w.at[s], narrow)


def prepare_out_body(w_out, w_out_o):
    reordered(w_out_o, slice(None), w_out, w_out.shape[0])


def put_pieces(spot, mine, y, core, both):
    narrow = mine.shape[1]
    for yl in range(2):

        @pl.when(lax.axis_index("yl") == yl)
        def _():
            for k, (near, far) in enumerate(((mine, y), (core, both))):
                for at, piece in ((2 * k + yl, near), (2 * k + 1 - yl, far)):
                    spot[:, at * narrow : (at + 1) * narrow] = piece[...]


def forward_body(z0, zy, zc, zcy, w, normal_o, xt_o, inv_o, qkv_o, probs_o, att_o, zs):
    put_pieces(zs, z0, zy, zc, zcy)
    width = zs.shape[1]
    narrow = width // 4
    values = zs[...].astype(f32)
    centred = values - jnp.sum(values, axis=-1, keepdims=True) * (1.0 / width)
    inv = lax.rsqrt(jnp.sum(centred * centred, axis=-1, keepdims=True) * (1.0 / width) + epsilon)
    inv_o[...] = jnp.broadcast_to(inv, inv_o.shape)
    normal_o[...] = (centred * inv).astype(bf16)
    heads = narrow // HD
    for s in range(3):
        got = dot(normal_o[...], w[s * narrow : (s + 1) * narrow, :], COLS).astype(bf16)
        for h in range(heads):
            qkv_o[s * heads + h] = got[:, h * HD : (h + 1) * HD]
    xt_o[...] = normal_o[...].T
    scores = [dot(qkv_o[h], qkv_o[heads + h], COLS) * SCALE for h in range(heads)]
    for h in range(heads):
        e = jnp.exp(scores[h] - jnp.max(scores[h], axis=-1, keepdims=True))
        probs_o[h] = e / jnp.sum(e, axis=-1, keepdims=True)
    for h in range(heads):
        att_o[:, h * HD : (h + 1) * HD] = dot(probs_o[h].astype(bf16), qkv_o[2 * heads + h]).astype(bf16)


def attention_back(cot, w_out, qkv, probs, grads):
    narrow = w_out.shape[0]
    heads = narrow // HD
    att = dot(cot, w_out[...], COLS).astype(bf16)
    each = [att[:, h * HD : (h + 1) * HD] for h in range(heads)]

    def put(s, h, got):
        at = s * narrow + h * HD
        grads[:, at : at + HD] = got.astype(bf16)

    dps = [dot(each[h], qkv[2 * heads + h], COLS) for h in range(heads)]
    for h in range(heads):
        put(2, h, dot(probs[h].astype(bf16), each[h], ROWS))
    for h in range(heads):
        p = probs[h]
        along = jnp.sum(p * dps[h], axis=-1, keepdims=True)
        ds = (p * (dps[h] - along) * SCALE).astype(bf16)
        put(0, h, dot(ds, qkv[heads + h]))
        put(1, h, dot(ds, qkv[h], ROWS))


def input_back(half, grads, w):
    wide = w.shape[1] // 2
    return dot(grads[...], w[:, half * wide : (half + 1) * wide]).astype(bf16)


def first_body(t0, ty, tc, tcy, w_out, qkv, probs, w, cot_o, grads_o, oth_o):
    put_pieces(cot_o, t0, ty, tc, tcy)
    attention_back(cot_o[...], w_out, qkv, probs, grads_o)
    oth_o[...] = input_back(OTHER, grads_o, w)


def own_body(grads, w, own_o):
    own_o[...] = input_back(MINE, grads, w)


def put_term(spot, chip, far, chip_c, far_c, normal, inv):
    half = chip.shape[1]
    spot[:, :half] = chip[...].astype(f32) + far[...].astype(f32)
    spot[:, half:] = chip_c[...].astype(f32) + far_c[...].astype(f32)
    g = spot[...]
    width = g.shape[1]
    n = normal[...].astype(f32)
    mean = jnp.sum(g, axis=-1, keepdims=True) * (1.0 / width)
    along = jnp.sum(g * n, axis=-1, keepdims=True) * (1.0 / width)
    return (g - mean - n * along) * inv[:, :1]


def middle_body(chip, far, chip_c, far_c, normal, inv, w_out, qkv, probs, w, term_o, grads_o, oth_o):
    term_o[...] = put_term(term_o, chip, far, chip_c, far_c, normal, inv)
    attention_back(term_o[...].astype(bf16), w_out, qkv, probs, grads_o)
    oth_o[...] = input_back(OTHER, grads_o, w)


def total_body(picks, chip, far, chip_c, far_c, normal, inv, cot, term, mine, att, imp_o, total_o, tt_o, out, spot, rows):
    spot[...] = put_term(spot, chip, far, chip_c, far_c, normal, inv) + term[...]
    narrow = mine.shape[1]
    for yl in range(2):

        @pl.when(lax.axis_index("yl") == yl)
        def _():
            imp_o[...] = mine[...] + spot[:, yl * narrow : (yl + 1) * narrow]

    total = (spot[...] + cot[...].astype(f32)).astype(bf16)
    total_o[...] = total
    tt_o[...] = total.T
    gather_rows(tt_o, rows, picks, narrow)
    out[...] = dot(rows[...], att[...]).astype(bf16)


def last_body(total, w_out, qkv, probs, one_o, two_o, grads):
    attention_back(total[...], w_out, qkv, probs, grads)
    cols = one_o.shape[1]
    one_o[...] = grads[:, :cols]
    two_o[...] = grads[:, cols:]


def spot_of(x, narrow):
    other = lax.rem(x + lax.axis_index("c"), 2)
    return (2 * other + lax.div(x, 2)) * narrow


def gather_rows(src, dst, picks, narrow):
    rows = narrow // 2
    for i, (dx, dy) in enumerate(picks):
        at = spot_of(lax.bitwise_xor(lax.axis_index("x"), dx), narrow)
        at = at + lax.bitwise_xor(lax.axis_index("yh"), dy) * rows
        dst[i * rows : (i + 1) * rows, :] = src[pl.ds(pl.multiple_of(at, 16), rows), :]


def pick_body(picks, xt, out):
    gather_rows(xt, out, picks, xt.shape[0] // 4)


def rows_body(picks, x, g, out, rows):
    gather_rows(x, rows, picks, x.shape[0] // 4)
    out[...] = dot(rows[...], g[...]).astype(out.dtype)


def both_body(start, mine, x, g, out):
    at = slice(start, start + out.shape[0])
    out[...] = (mine[at, :] + dot(x[at, :], g[...])).astype(bf16)


def pack_body(k1, g1, k2, g2, k3, g3, out, spot):
    at = 0
    for k, g in ((k1, g1), (k2, g2), (k3, g3)):
        spot[:, at : at + k.shape[1]] = k[...].astype(f32) + g[...].astype(f32)
        at += k.shape[1]
    nz, _, lanes = out.shape
    each = spot.shape[0] // nz
    for z in range(nz):
        for b in range(spot.shape[1] // lanes):
            piece = spot[z * each : (z + 1) * each, b * lanes : (b + 1) * lanes]
            out[z, b * each : (b + 1) * each, :] = piece.astype(bf16)


def unpack_body(factor, got, qkv_o, out_o, spot):
    total = got[0].astype(f32)
    for z in range(1, got.shape[0]):
        total = total + got[z].astype(f32)
    total = total * factor
    each, width = spot.shape
    lanes = got.shape[2]
    for b in range(width // lanes):
        spot[:, b * lanes : (b + 1) * lanes] = total[b * each : (b + 1) * each, :]
    narrow = out_o.shape[1]
    for k in range(3):
        qkv_o[k] = spot[:, k * narrow : (k + 1) * narrow]
    out_o[...] = spot[:, 3 * narrow :]


def add(*parts):
    return sum(p.astype(f32) for p in parts).astype(bf16)


def mp_sum(oth, own):
    chip = add(own(), lax.ppermute(oth, "c", SWAP))
    far = lax.ppermute(chip, "yl", SWAP)
    far_c = lax.ppermute(far, "c", SWAP)
    return chip, far, lax.ppermute(chip, "c", SWAP), far_c


def shards(z_star, cotangent, w_qkv, w_out):
    images, tokens, narrow = z_star.shape
    width = 4 * narrow
    heads = narrow // HD
    nx, ny, nz = [lax.axis_size(a) for a in DP]

    wide = like((tokens, width), bf16)
    wide_f = like((tokens, width), f32)
    half = like((tokens, 2 * narrow), bf16)
    g_like = like((tokens, 3 * narrow), bf16)
    proj = 2 * tokens * width * narrow
    small = 2 * tokens * tokens * HD * heads

    z0 = z_star[0]
    zy = lax.ppermute(z0, "yl", SWAP)
    zc = lax.ppermute(z0, "c", SWAP)
    t0, w = call(
        prepare_body,
        (like((tokens, narrow), bf16), like((3 * narrow, width), bf16)),
        (cotangent[0], jnp.swapaxes(w_qkv, 1, 2)),
        flops=proj,
    )
    (wo,) = call(prepare_out_body, (like((narrow, width), bf16),), (w_out,), flops=proj)
    tc = lax.ppermute(t0, "c", SWAP)
    zcy = lax.ppermute(zy, "c", SWAP)
    ty = lax.ppermute(t0, "yl", SWAP)
    tcy = lax.ppermute(ty, "c", SWAP)
    normal, xt, inv, qkv, probs, att = call(
        forward_body,
        (
            wide,
            like((width, tokens), bf16),
            like((tokens, 128), f32),
            like((3 * heads, tokens, HD), bf16),
            like((heads, tokens, tokens), f32),
            like((tokens, narrow), bf16),
        ),
        (z0, zy, zc, zcy, w),
        [pltpu.VMEM((tokens, width), bf16)],
        flops=3 * proj + 2 * small,
    )

    def own_of(grads):
        return call(own_body, (half,), (grads, w), flops=3 * proj // 2)[0]

    cot, grads, oth = call(
        first_body,
        (wide, g_like, half),
        (t0, ty, tc, tcy, wo, qkv, probs, w),
        flops=3 * proj + 4 * small,
    )
    sums = mp_sum(oth, lambda: own_of(grads))
    term, grads, oth = call(
        middle_body,
        (wide_f, g_like, half),
        (*sums, normal, inv, wo, qkv, probs, w),
        flops=3 * proj + 4 * small,
    )
    sums = mp_sum(oth, lambda: own_of(grads))

    rows = width // (nx * ny)
    each = rows // nz
    tall = pltpu.VMEM((4 * rows, tokens), bf16)
    tall_like = like((4 * rows, tokens), bf16)
    one, two, three = 448, 512, narrow
    give_one = ((1, 0), (1, 1), (2, 0), (2, 1))
    keep_one = ((0, 0), (0, 1), (3, 0), (3, 1))
    give_two = ((3, 0), (2, 0), (3, 1), (2, 1))
    keep_two = ((0, 0), (1, 0), (0, 1), (1, 1))
    give_three = ((0, 1), (3, 1), (1, 1), (2, 1))
    keep_three = ((0, 0), (3, 0), (1, 0), (2, 0))

    def swap_x(value, by):
        return lax.ppermute(value, "x", [(i, i ^ by) for i in range(nx)])

    def swap_yh(value):
        return lax.ppermute(value, "yh", SWAP)

    def pick(picks):
        body = functools.partial(pick_body, picks)
        (part,) = call(body, (tall_like,), (xt,), flops=proj)
        return part

    x_two = swap_x(pick(give_two), 3)
    x_one = swap_x(pick(give_one), 1)

    implicit, total, tt, s3 = call(
        functools.partial(total_body, give_three),
        (
            like((tokens, narrow), f32),
            wide,
            like((width, tokens), bf16),
            like((4 * rows, three), bf16),
        ),
        (*sums, normal, inv, cot, term, cotangent[0], att),
        [pltpu.VMEM((tokens, width), f32), tall],
        flops=proj,
    )
    g3 = swap_yh(s3)
    g_one, g_two = call(
        last_body,
        (like((tokens, one), bf16), like((tokens, two), bf16)),
        (total, wo, qkv, probs),
        [pltpu.VMEM((tokens, 3 * narrow), bf16)],
        flops=proj + 4 * small,
    )
    p_two = swap_x(g_two, 3)
    p_one = swap_x(g_one, 1)

    def block(picks, x, g, dtype):
        cols = g.shape[1]
        return call(
            functools.partial(rows_body, picks),
            (like((4 * rows, cols), dtype),),
            (x, g),
            [tall],
            flops=2 * tokens * 4 * rows * cols,
        )[0]

    def both(start, mine, x, g):
        return call(
            functools.partial(both_body, start * rows),
            (like((2 * rows, g.shape[1]), bf16),),
            (mine, x, g),
            flops=2 * tokens * 2 * rows * g.shape[1],
        )[0]

    m2 = block(keep_two, xt, g_two, f32)
    m1 = block(keep_one, xt, g_one, f32)
    k3 = block(keep_three, tt, att, bf16)

    def at(value, start, count):
        return value[start * rows : (start + count) * rows]

    h2 = swap_yh(both(2, m2, x_two, p_two))
    h1 = swap_x(both(2, m1, x_one, p_one), 3)
    h3 = swap_x(add(at(k3, 2, 2), at(g3, 2, 2)), 1)
    k2 = both(0, m2, x_two, p_two)
    k1 = both(0, m1, x_one, p_one)
    k3 = add(at(k3, 0, 2), at(g3, 0, 2))

    def last_half(k, h, swap):
        got = swap(add(at(k, 1, 1), at(h, 1, 1)))
        return add(at(k, 0, 1), at(h, 0, 1)), got

    e2 = last_half(k2, h2, lambda v: swap_x(v, 1))
    e1 = last_half(k1, h1, swap_yh)
    e3 = last_half(k3, h3, lambda v: swap_x(v, 3))
    dense = each * width // 128
    (packed,) = call(
        pack_body,
        (like((nz, dense, 128), bf16),),
        (*e1, *e2, *e3),
        [pltpu.VMEM((rows, width), f32)],
        flops=rows * width,
    )
    got = lax.all_to_all(packed, "z", 0, 0, tiled=True)
    factor = 1.0 / math.sqrt(images * nx * ny * nz * tokens)
    grad_qkv, grad_o = call(
        functools.partial(unpack_body, factor),
        (like((3, each, narrow), f32), like((each, narrow), f32)),
        (got,),
        [pltpu.VMEM((each, width), f32)],
        flops=rows * width,
    )
    return implicit[None], grad_qkv, grad_o.T


def solution(mesh):
    split = Mesh(mesh.devices.reshape(4, 2, 8, 2, 2), AXES)

    return jax.shard_map(
        shards,
        mesh=split,
        in_specs=(P(DP, None, MP), P(DP, None, MP), P(None, None, MP), P(MP, None)),
        out_specs=(P(DP, None, MP), P(None, DP, MP), P(MP, DP)),
        check_vma=False,
    )
```

```python
import functools
import math

import jax
import jax.numpy as jnp
from jax import lax
from jax.experimental import pallas as pl
from jax.experimental.pallas import tpu as pltpu
from jax.sharding import Mesh
from jax.sharding import PartitionSpec as P


HD = 80
AXES = ("x", "yh", "z", "yl", "c")
DP = ("x", "yh", "z")
MP = ("yl", "c")
SWAP = [(0, 1), (1, 0)]
MINE, OTHER = 0, 1

epsilon = 1e-06
f32 = jnp.float32
bf16 = jnp.bfloat16
SCALE = HD ** (-0.5)
ROWS = (((0,), (0,)), ((), ()))
COLS = (((1,), (1,)), ((), ()))


def dot(a, b, dims=(((1,), (0,)), ((), ()))):
    return lax.dot_general(a, b, dims, preferred_element_type=f32)


def call(body, outs, ins, scratch=(), flops=0):
    vmem = pl.BlockSpec(memory_space=pltpu.VMEM)
    size = sum(math.prod(o.shape) * o.dtype.itemsize for o in list(outs) + list(ins))
    return pl.pallas_call(
        body,
        out_shape=outs,
        in_specs=[vmem] * len(ins),
        out_specs=[vmem] * len(outs),
        scratch_shapes=list(scratch),
        compiler_params=pltpu.CompilerParams(vmem_limit_bytes=20 * 2**20),
        cost_estimate=pl.CostEstimate(flops=flops, bytes_accessed=size, transcendentals=0),
    )(*ins)


def like(shape, dtype):
    return jax.ShapeDtypeStruct(shape, dtype)


def reordered(dst, rows, src, narrow):
    for c in range(2):

        @pl.when(lax.axis_index("c") == c)
        def _():
            for k, core in enumerate((c, 1 - c)):
                for y in range(2):
                    old = (2 * y + core) * narrow
                    new = (2 * k + y) * narrow
                    dst[rows, new : new + narrow] = src[:, old : old + narrow]


def prepare_body(cot, w, cot_o, w_o):
    narrow = cot.shape[1]
    cot_o[...] = cot[...].astype(bf16)
    for s in range(3):
        reordered(w_o, slice(s * narrow, (s + 1) * narrow), w.at[s], narrow)


def prepare_out_body(w_out, w_out_o):
    reordered(w_out_o, slice(None), w_out, w_out.shape[0])


def put_pieces(spot, mine, y, core, both):
    narrow = mine.shape[1]
    for yl in range(2):

        @pl.when(lax.axis_index("yl") == yl)
        def _():
            for k, (near, far) in enumerate(((mine, y), (core, both))):
                for at, piece in ((2 * k + yl, near), (2 * k + 1 - yl, far)):
                    spot[:, at * narrow : (at + 1) * narrow] = piece[...]


def forward_body(z0, zy, zc, zcy, w, normal_o, xt_o, inv_o, qkv_o, probs_o, att_o, zs):
    put_pieces(zs, z0, zy, zc, zcy)
    width = zs.shape[1]
    narrow = width // 4
    values = zs[...].astype(f32)
    centred = values - jnp.sum(values, axis=-1, keepdims=True) * (1.0 / width)
    inv = lax.rsqrt(jnp.sum(centred * centred, axis=-1, keepdims=True) * (1.0 / width) + epsilon)
    inv_o[...] = jnp.broadcast_to(inv, inv_o.shape)
    normal_o[...] = (centred * inv).astype(bf16)
    heads = narrow // HD
    for s in range(3):
        got = dot(normal_o[...], w[s * narrow : (s + 1) * narrow, :], COLS).astype(bf16)
        for h in range(heads):
            qkv_o[s * heads + h] = got[:, h * HD : (h + 1) * HD]
    xt_o[...] = normal_o[...].T
    scores = [dot(qkv_o[h], qkv_o[heads + h], COLS) * SCALE for h in range(heads)]
    for h in range(heads):
        e = jnp.exp(scores[h] - jnp.max(scores[h], axis=-1, keepdims=True))
        probs_o[h] = e / jnp.sum(e, axis=-1, keepdims=True)
    for h in range(heads):
        att_o[:, h * HD : (h + 1) * HD] = dot(probs_o[h].astype(bf16), qkv_o[2 * heads + h]).astype(bf16)


def attention_back(cot, w_out, qkv, probs, grads):
    narrow = w_out.shape[0]
    heads = narrow // HD
    att = dot(cot, w_out[...], COLS).astype(bf16)
    each = [att[:, h * HD : (h + 1) * HD] for h in range(heads)]

    def put(s, h, got):
        at = s * narrow + h * HD
        grads[:, at : at + HD] = got.astype(bf16)

    dps = [dot(each[h], qkv[2 * heads + h], COLS) for h in range(heads)]
    for h in range(heads):
        put(2, h, dot(probs[h].astype(bf16), each[h], ROWS))
    for h in range(heads):
        p = probs[h]
        along = jnp.sum(p * dps[h], axis=-1, keepdims=True)
        ds = (p * (dps[h] - along) * SCALE).astype(bf16)
        put(0, h, dot(ds, qkv[heads + h]))
        put(1, h, dot(ds, qkv[h], ROWS))


def input_back(half, grads, w):
    wide = w.shape[1] // 2
    return dot(grads[...], w[:, half * wide : (half + 1) * wide]).astype(bf16)


def first_body(t0, ty, tc, tcy, w_out, qkv, probs, w, cot_o, grads_o, oth_o):
    put_pieces(cot_o, t0, ty, tc, tcy)
    attention_back(cot_o[...], w_out, qkv, probs, grads_o)
    oth_o[...] = input_back(OTHER, grads_o, w)


def own_body(grads, w, own_o):
    own_o[...] = input_back(MINE, grads, w)


def put_term(spot, chip, far, chip_c, far_c, normal, inv):
    half = chip.shape[1]
    spot[:, :half] = chip[...].astype(f32) + far[...].astype(f32)
    spot[:, half:] = chip_c[...].astype(f32) + far_c[...].astype(f32)
    g = spot[...]
    width = g.shape[1]
    n = normal[...].astype(f32)
    mean = jnp.sum(g, axis=-1, keepdims=True) * (1.0 / width)
    along = jnp.sum(g * n, axis=-1, keepdims=True) * (1.0 / width)
    return (g - mean - n * along) * inv[:, :1]


def middle_body(chip, far, chip_c, far_c, normal, inv, w_out, qkv, probs, w, term_o, grads_o, oth_o):
    term_o[...] = put_term(term_o, chip, far, chip_c, far_c, normal, inv)
    attention_back(term_o[...].astype(bf16), w_out, qkv, probs, grads_o)
    oth_o[...] = input_back(OTHER, grads_o, w)


LANES = 128
PART = 160


def folded(cols):
    return PART * cols // LANES


def fold(out, value):
    rows, cols = value.shape
    size = folded(cols)
    whole = cols // LANES
    for p in range(rows // PART):
        top, base = p * PART, p * size
        for b in range(whole):
            block = value[top : top + PART, b * LANES : (b + 1) * LANES]
            out[base + b * PART : base + (b + 1) * PART, :] = block.astype(out.dtype)
        if cols % LANES:
            base += whole * PART
            for k in range(2):
                block = value[top + k * PART // 2 : top + (k + 1) * PART // 2, whole * LANES :]
                out[base : base + PART // 2, k * LANES // 2 : (k + 1) * LANES // 2] = block.astype(out.dtype)


def unfold(out, at, value, cols):
    whole = cols // LANES
    for b in range(whole):
        out[:, at + b * LANES : at + (b + 1) * LANES] = value[b * PART : (b + 1) * PART, :]
    if cols % LANES:
        at += whole * LANES
        for k in range(2):
            block = value[whole * PART :, k * LANES // 2 : (k + 1) * LANES // 2]
            out[k * PART // 2 : (k + 1) * PART // 2, at : at + LANES // 2] = block


def total_body(picks, chip, far, chip_c, far_c, normal, inv, cot, term, mine, att, imp_o, total_o, tt_o, out, spot, rows):
    spot[...] = put_term(spot, chip, far, chip_c, far_c, normal, inv) + term[...]
    narrow = mine.shape[1]
    for yl in range(2):

        @pl.when(lax.axis_index("yl") == yl)
        def _():
            imp_o[...] = mine[...] + spot[:, yl * narrow : (yl + 1) * narrow]

    total = (spot[...] + cot[...].astype(f32)).astype(bf16)
    total_o[...] = total
    tt_o[...] = total.T
    gather_rows(tt_o, rows, picks, narrow)
    fold(out, dot(rows[...], att[...]))


def last_body(total, w_out, qkv, probs, one_o, two_o, grads):
    attention_back(total[...], w_out, qkv, probs, grads)
    cols = one_o.shape[1]
    one_o[...] = grads[:, :cols]
    two_o[...] = grads[:, cols:]


def spot_of(x, narrow):
    other = lax.rem(x + lax.axis_index("c"), 2)
    return (2 * other + lax.div(x, 2)) * narrow


def gather_rows(src, dst, picks, narrow):
    rows = narrow // 2
    for i, (dx, dy) in enumerate(picks):
        at = spot_of(lax.bitwise_xor(lax.axis_index("x"), dx), narrow)
        at = at + lax.bitwise_xor(lax.axis_index("yh"), dy) * rows
        dst[i * rows : (i + 1) * rows, :] = src[pl.ds(pl.multiple_of(at, 16), rows), :]


def pick_body(picks, xt, out):
    gather_rows(xt, out, picks, xt.shape[0] // 4)


def rows_body(picks, x, g, out, rows):
    gather_rows(x, rows, picks, x.shape[0] // 4)
    out[...] = dot(rows[...], g[...]).astype(out.dtype)


def folded_rows_body(picks, x, g, out, rows):
    gather_rows(x, rows, picks, x.shape[0] // 4)
    fold(out, dot(rows[...], g[...]))


def both_body(start, mine, x, g, out):
    at = slice(start, start + x.shape[0] // 2)
    fold(out, mine[at, :] + dot(x[at, :], g[...]))


def pack_body(widths, k1, g1, k2, g2, k3, g3, out, spot):
    at = 0
    for cols, k, g in zip(widths, (k1, k2, k3), (g1, g2, g3)):
        unfold(spot, at, k[...].astype(f32) + g[...].astype(f32), cols)
        at += cols
    nz, _, lanes = out.shape
    each = spot.shape[0] // nz
    for z in range(nz):
        for b in range(spot.shape[1] // lanes):
            piece = spot[z * each : (z + 1) * each, b * lanes : (b + 1) * lanes]
            out[z, b * each : (b + 1) * each, :] = piece.astype(bf16)


def unpack_body(factor, got, qkv_o, out_o, spot):
    total = got[0].astype(f32)
    for z in range(1, got.shape[0]):
        total = total + got[z].astype(f32)
    total = total * factor
    each, width = spot.shape
    lanes = got.shape[2]
    for b in range(width // lanes):
        spot[:, b * lanes : (b + 1) * lanes] = total[b * each : (b + 1) * each, :]
    narrow = out_o.shape[1]
    for k in range(3):
        qkv_o[k] = spot[:, k * narrow : (k + 1) * narrow]
    out_o[...] = spot[:, 3 * narrow :]


def add(*parts):
    return sum(p.astype(f32) for p in parts).astype(bf16)


def mp_sum(oth, own):
    chip = add(own(), lax.ppermute(oth, "c", SWAP))
    far = lax.ppermute(chip, "yl", SWAP)
    far_c = lax.ppermute(far, "c", SWAP)
    return chip, far, lax.ppermute(chip, "c", SWAP), far_c


def shards(z_star, cotangent, w_qkv, w_out):
    images, tokens, narrow = z_star.shape
    width = 4 * narrow
    heads = narrow // HD
    nx, ny, nz = [lax.axis_size(a) for a in DP]

    wide = like((tokens, width), bf16)
    wide_f = like((tokens, width), f32)
    half = like((tokens, 2 * narrow), bf16)
    g_like = like((tokens, 3 * narrow), bf16)
    proj = 2 * tokens * width * narrow
    small = 2 * tokens * tokens * HD * heads

    z0 = z_star[0]
    zy = lax.ppermute(z0, "yl", SWAP)
    zc = lax.ppermute(z0, "c", SWAP)
    t0, w = call(
        prepare_body,
        (like((tokens, narrow), bf16), like((3 * narrow, width), bf16)),
        (cotangent[0], jnp.swapaxes(w_qkv, 1, 2)),
        flops=proj,
    )
    (wo,) = call(prepare_out_body, (like((narrow, width), bf16),), (w_out,), flops=proj)
    tc = lax.ppermute(t0, "c", SWAP)
    zcy = lax.ppermute(zy, "c", SWAP)
    ty = lax.ppermute(t0, "yl", SWAP)
    tcy = lax.ppermute(ty, "c", SWAP)
    normal, xt, inv, qkv, probs, att = call(
        forward_body,
        (
            wide,
            like((width, tokens), bf16),
            like((tokens, 128), f32),
            like((3 * heads, tokens, HD), bf16),
            like((heads, tokens, tokens), f32),
            like((tokens, narrow), bf16),
        ),
        (z0, zy, zc, zcy, w),
        [pltpu.VMEM((tokens, width), bf16)],
        flops=3 * proj + 2 * small,
    )

    def own_of(grads):
        return call(own_body, (half,), (grads, w), flops=3 * proj // 2)[0]

    cot, grads, oth = call(
        first_body,
        (wide, g_like, half),
        (t0, ty, tc, tcy, wo, qkv, probs, w),
        flops=3 * proj + 4 * small,
    )
    sums = mp_sum(oth, lambda: own_of(grads))
    term, grads, oth = call(
        middle_body,
        (wide_f, g_like, half),
        (*sums, normal, inv, wo, qkv, probs, w),
        flops=3 * proj + 4 * small,
    )
    sums = mp_sum(oth, lambda: own_of(grads))

    rows = width // (nx * ny)
    each = rows // nz
    tall = pltpu.VMEM((4 * rows, tokens), bf16)
    tall_like = like((4 * rows, tokens), bf16)
    one, two, three = 448, 512, narrow
    give_one = ((1, 0), (1, 1), (2, 0), (2, 1))
    keep_one = ((0, 0), (0, 1), (3, 0), (3, 1))
    give_two = ((3, 0), (2, 0), (3, 1), (2, 1))
    keep_two = ((0, 0), (1, 0), (0, 1), (1, 1))
    give_three = ((0, 1), (3, 1), (1, 1), (2, 1))
    keep_three = ((0, 0), (3, 0), (1, 0), (2, 0))

    def swap_x(value, by):
        return lax.ppermute(value, "x", [(i, i ^ by) for i in range(nx)])

    def swap_yh(value):
        return lax.ppermute(value, "yh", SWAP)

    def pick(picks):
        body = functools.partial(pick_body, picks)
        (part,) = call(body, (tall_like,), (xt,), flops=proj)
        return part

    x_two = swap_x(pick(give_two), 3)
    x_one = swap_x(pick(give_one), 1)

    implicit, total, tt, s3 = call(
        functools.partial(total_body, give_three),
        (
            like((tokens, narrow), f32),
            wide,
            like((width, tokens), bf16),
            like((4 * folded(three), LANES), bf16),
        ),
        (*sums, normal, inv, cot, term, cotangent[0], att),
        [pltpu.VMEM((tokens, width), f32), tall],
        flops=proj,
    )
    g3 = swap_yh(s3)
    g_one, g_two = call(
        last_body,
        (like((tokens, one), bf16), like((tokens, two), bf16)),
        (total, wo, qkv, probs),
        [pltpu.VMEM((tokens, 3 * narrow), bf16)],
        flops=proj + 4 * small,
    )
    p_two = swap_x(g_two, 3)
    p_one = swap_x(g_one, 1)

    def block(picks, x, g, dtype):
        cols = g.shape[1]
        return call(
            functools.partial(rows_body, picks),
            (like((4 * rows, cols), dtype),),
            (x, g),
            [tall],
            flops=2 * tokens * 4 * rows * cols,
        )[0]

    def both(start, mine, x, g):
        return call(
            functools.partial(both_body, start * rows),
            (like((2 * folded(g.shape[1]), LANES), bf16),),
            (mine, x, g),
            flops=2 * tokens * 2 * rows * g.shape[1],
        )[0]

    m2 = block(keep_two, xt, g_two, f32)
    m1 = block(keep_one, xt, g_one, f32)
    (k3,) = call(
        functools.partial(folded_rows_body, keep_three),
        (like((4 * folded(three), LANES), bf16),),
        (tt, att),
        [tall],
        flops=2 * tokens * 4 * rows * three,
    )

    def at(value, start, count, parts):
        size = value.shape[0] // parts
        return value[start * size : (start + count) * size]

    h2 = swap_yh(both(2, m2, x_two, p_two))
    h1 = swap_x(both(2, m1, x_one, p_one), 3)
    h3 = swap_x(add(at(k3, 2, 2, 4), at(g3, 2, 2, 4)), 1)
    k2 = both(0, m2, x_two, p_two)
    k1 = both(0, m1, x_one, p_one)
    k3 = add(at(k3, 0, 2, 4), at(g3, 0, 2, 4))

    def last_half(k, h, swap):
        got = swap(add(at(k, 1, 1, 2), at(h, 1, 1, 2)))
        return add(at(k, 0, 1, 2), at(h, 0, 1, 2)), got

    e2 = last_half(k2, h2, lambda v: swap_x(v, 1))
    e1 = last_half(k1, h1, swap_yh)
    e3 = last_half(k3, h3, lambda v: swap_x(v, 3))
    dense = each * width // 128
    (packed,) = call(
        functools.partial(pack_body, (one, two, three)),
        (like((nz, dense, 128), bf16),),
        (*e1, *e2, *e3),
        [pltpu.VMEM((rows, width), f32)],
        flops=rows * width,
    )
    got = lax.all_to_all(packed, "z", 0, 0, tiled=True)
    factor = 1.0 / math.sqrt(images * nx * ny * nz * tokens)
    grad_qkv, grad_o = call(
        functools.partial(unpack_body, factor),
        (like((3, each, narrow), f32), like((each, narrow), f32)),
        (got,),
        [pltpu.VMEM((each, width), f32)],
        flops=rows * width,
    )
    return implicit[None], grad_qkv, grad_o.T


def solution(mesh):
    split = Mesh(mesh.devices.reshape(4, 2, 8, 2, 2), AXES)

    return jax.shard_map(
        shards,
        mesh=split,
        in_specs=(P(DP, None, MP), P(DP, None, MP), P(None, None, MP), P(MP, None)),
        out_specs=(P(DP, None, MP), P(None, DP, MP), P(MP, DP)),
        check_vma=False,
    )
```

```python
import functools
import math

import jax
import jax.numpy as jnp
from jax import lax
from jax.experimental import pallas as pl
from jax.experimental.pallas import tpu as pltpu
from jax.sharding import Mesh
from jax.sharding import PartitionSpec as P


HD = 80
AXES = ("x", "yh", "z", "yl", "c")
DP = ("x", "yh", "z")
MP = ("yl", "c")
SWAP = [(0, 1), (1, 0)]
MINE, OTHER = 0, 1

epsilon = 1e-06
f32 = jnp.float32
bf16 = jnp.bfloat16
SCALE = HD ** (-0.5)
ROWS = (((0,), (0,)), ((), ()))
COLS = (((1,), (1,)), ((), ()))


def dot(a, b, dims=(((1,), (0,)), ((), ()))):
    return lax.dot_general(a, b, dims, preferred_element_type=f32)


def call(body, outs, ins, scratch=(), flops=0):
    vmem = pl.BlockSpec(memory_space=pltpu.VMEM)
    size = sum(math.prod(o.shape) * o.dtype.itemsize for o in list(outs) + list(ins))
    return pl.pallas_call(
        body,
        out_shape=outs,
        in_specs=[vmem] * len(ins),
        out_specs=[vmem] * len(outs),
        scratch_shapes=list(scratch),
        compiler_params=pltpu.CompilerParams(vmem_limit_bytes=20 * 2**20),
        cost_estimate=pl.CostEstimate(flops=flops, bytes_accessed=size, transcendentals=0),
    )(*ins)


def like(shape, dtype):
    return jax.ShapeDtypeStruct(shape, dtype)


def reordered(dst, rows, src, narrow):
    for c in range(2):

        @pl.when(lax.axis_index("c") == c)
        def _():
            for k, core in enumerate((c, 1 - c)):
                for y in range(2):
                    old = (2 * y + core) * narrow
                    new = (2 * k + y) * narrow
                    dst[rows, new : new + narrow] = src[:, old : old + narrow]


def prepare_body(cot, w, cot_o, w_o):
    narrow = cot.shape[1]
    cot_o[...] = cot[...].astype(bf16)
    for s in range(3):
        reordered(w_o, slice(s * narrow, (s + 1) * narrow), w.at[s], narrow)


def prepare_out_body(w_out, w_out_o):
    reordered(w_out_o, slice(None), w_out, w_out.shape[0])


def put_pieces(spot, mine, y, core, both):
    narrow = mine.shape[1]
    for yl in range(2):

        @pl.when(lax.axis_index("yl") == yl)
        def _():
            for k, (near, far) in enumerate(((mine, y), (core, both))):
                for at, piece in ((2 * k + yl, near), (2 * k + 1 - yl, far)):
                    spot[:, at * narrow : (at + 1) * narrow] = piece[...]


def forward_body(z0, zy, zc, zcy, w, normal_o, xt_o, inv_o, qkv_o, probs_o, att_o, zs):
    put_pieces(zs, z0, zy, zc, zcy)
    width = zs.shape[1]
    narrow = width // 4
    values = zs[...].astype(f32)
    centred = values - jnp.sum(values, axis=-1, keepdims=True) * (1.0 / width)
    inv = lax.rsqrt(jnp.sum(centred * centred, axis=-1, keepdims=True) * (1.0 / width) + epsilon)
    inv_o[...] = jnp.broadcast_to(inv, inv_o.shape)
    normal_o[...] = (centred * inv).astype(bf16)
    heads = narrow // HD
    for s in range(3):
        got = dot(normal_o[...], w[s * narrow : (s + 1) * narrow, :], COLS).astype(bf16)
        for h in range(heads):
            qkv_o[s * heads + h] = got[:, h * HD : (h + 1) * HD]
    xt_o[...] = normal_o[...].T
    scores = [dot(qkv_o[h], qkv_o[heads + h], COLS) * SCALE for h in range(heads)]
    for h in range(heads):
        e = jnp.exp(scores[h] - jnp.max(scores[h], axis=-1, keepdims=True))
        probs_o[h] = e / jnp.sum(e, axis=-1, keepdims=True)
    for h in range(heads):
        att_o[:, h * HD : (h + 1) * HD] = dot(probs_o[h].astype(bf16), qkv_o[2 * heads + h]).astype(bf16)


def attention_back(cot, w_out, qkv, probs, grads):
    narrow = w_out.shape[0]
    heads = narrow // HD
    att = dot(cot, w_out[...], COLS).astype(bf16)
    each = [att[:, h * HD : (h + 1) * HD] for h in range(heads)]

    def put(s, h, got):
        at = s * narrow + h * HD
        grads[:, at : at + HD] = got.astype(bf16)

    dps = [dot(each[h], qkv[2 * heads + h], COLS) for h in range(heads)]
    dss = []
    for h in range(heads):
        p = probs[h]
        along = jnp.sum(p * dps[h], axis=-1, keepdims=True)
        dss.append((p * (dps[h] - along) * SCALE).astype(bf16))
        put(2, h, dot(probs[h].astype(bf16), each[h], ROWS))
    for h in range(heads):
        put(0, h, dot(dss[h], qkv[heads + h]))
    for h in range(heads):
        put(1, h, dot(dss[h], qkv[h], ROWS))


def input_back(half, grads, w):
    wide = w.shape[1] // 2
    return dot(grads[...], w[:, half * wide : (half + 1) * wide]).astype(bf16)


def first_body(t0, ty, tc, tcy, w_out, qkv, probs, w, cot_o, grads_o, oth_o):
    put_pieces(cot_o, t0, ty, tc, tcy)
    attention_back(cot_o[...], w_out, qkv, probs, grads_o)
    oth_o[...] = input_back(OTHER, grads_o, w)


def own_body(grads, w, own_o):
    own_o[...] = input_back(MINE, grads, w)


def put_term(spot, chip, far, chip_c, far_c, normal, inv):
    half = chip.shape[1]
    spot[:, :half] = chip[...].astype(f32) + far[...].astype(f32)
    spot[:, half:] = chip_c[...].astype(f32) + far_c[...].astype(f32)
    g = spot[...]
    width = g.shape[1]
    n = normal[...].astype(f32)
    mean = jnp.sum(g, axis=-1, keepdims=True) * (1.0 / width)
    along = jnp.sum(g * n, axis=-1, keepdims=True) * (1.0 / width)
    return (g - mean - n * along) * inv[:, :1]


def middle_body(chip, far, chip_c, far_c, normal, inv, w_out, qkv, probs, w, term_o, grads_o, oth_o):
    term_o[...] = put_term(term_o, chip, far, chip_c, far_c, normal, inv)
    attention_back(term_o[...].astype(bf16), w_out, qkv, probs, grads_o)
    oth_o[...] = input_back(OTHER, grads_o, w)


LANES = 128
PART = 160


def folded(cols):
    return PART * cols // LANES


def fold(out, value):
    rows, cols = value.shape
    size = folded(cols)
    whole = cols // LANES
    for p in range(rows // PART):
        top, base = p * PART, p * size
        for b in range(whole):
            block = value[top : top + PART, b * LANES : (b + 1) * LANES]
            out[base + b * PART : base + (b + 1) * PART, :] = block.astype(out.dtype)
        if cols % LANES:
            base += whole * PART
            for k in range(2):
                block = value[top + k * PART // 2 : top + (k + 1) * PART // 2, whole * LANES :]
                out[base : base + PART // 2, k * LANES // 2 : (k + 1) * LANES // 2] = block.astype(out.dtype)


def unfold(out, at, value, cols):
    whole = cols // LANES
    for b in range(whole):
        out[:, at + b * LANES : at + (b + 1) * LANES] = value[b * PART : (b + 1) * PART, :]
    if cols % LANES:
        at += whole * LANES
        for k in range(2):
            block = value[whole * PART :, k * LANES // 2 : (k + 1) * LANES // 2]
            out[k * PART // 2 : (k + 1) * PART // 2, at : at + LANES // 2] = block


def total_body(picks, chip, far, chip_c, far_c, normal, inv, cot, term, mine, att, imp_o, total_o, tt_o, out, spot, rows):
    spot[...] = put_term(spot, chip, far, chip_c, far_c, normal, inv) + term[...]
    narrow = mine.shape[1]
    for yl in range(2):

        @pl.when(lax.axis_index("yl") == yl)
        def _():
            imp_o[...] = mine[...] + spot[:, yl * narrow : (yl + 1) * narrow]

    total = (spot[...] + cot[...].astype(f32)).astype(bf16)
    total_o[...] = total
    tt_o[...] = total.T
    gather_rows(tt_o, rows, picks, narrow)
    fold(out, dot(rows[...], att[...]))


def last_body(total, w_out, qkv, probs, one_o, two_o, grads):
    attention_back(total[...], w_out, qkv, probs, grads)
    cols = one_o.shape[1]
    one_o[...] = grads[:, :cols]
    two_o[...] = grads[:, cols:]


def spot_of(x, narrow):
    other = lax.rem(x + lax.axis_index("c"), 2)
    return (2 * other + lax.div(x, 2)) * narrow


def gather_rows(src, dst, picks, narrow):
    rows = narrow // 2
    for i, (dx, dy) in enumerate(picks):
        at = spot_of(lax.bitwise_xor(lax.axis_index("x"), dx), narrow)
        at = at + lax.bitwise_xor(lax.axis_index("yh"), dy) * rows
        dst[i * rows : (i + 1) * rows, :] = src[pl.ds(pl.multiple_of(at, 16), rows), :]


def pick_body(picks, xt, out):
    gather_rows(xt, out, picks, xt.shape[0] // 4)


def rows_body(picks, x, g, out, rows):
    gather_rows(x, rows, picks, x.shape[0] // 4)
    out[...] = dot(rows[...], g[...]).astype(out.dtype)


def folded_rows_body(picks, x, g, out, rows):
    gather_rows(x, rows, picks, x.shape[0] // 4)
    fold(out, dot(rows[...], g[...]))


def both_body(start, mine, x, g, out):
    at = slice(start, start + x.shape[0] // 2)
    fold(out, mine[at, :] + dot(x[at, :], g[...]))


def pack_body(widths, k1, g1, k2, g2, k3, g3, out, spot):
    at = 0
    for cols, k, g in zip(widths, (k1, k2, k3), (g1, g2, g3)):
        unfold(spot, at, k[...].astype(f32) + g[...].astype(f32), cols)
        at += cols
    nz, _, lanes = out.shape
    each = spot.shape[0] // nz
    for z in range(nz):
        for b in range(spot.shape[1] // lanes):
            piece = spot[z * each : (z + 1) * each, b * lanes : (b + 1) * lanes]
            out[z, b * each : (b + 1) * each, :] = piece.astype(bf16)


def unpack_body(factor, got, qkv_o, out_o, spot):
    total = got[0].astype(f32)
    for z in range(1, got.shape[0]):
        total = total + got[z].astype(f32)
    total = total * factor
    each, width = spot.shape
    lanes = got.shape[2]
    for b in range(width // lanes):
        spot[:, b * lanes : (b + 1) * lanes] = total[b * each : (b + 1) * each, :]
    narrow = out_o.shape[1]
    for k in range(3):
        qkv_o[k] = spot[:, k * narrow : (k + 1) * narrow]
    out_o[...] = spot[:, 3 * narrow :]


def add(*parts):
    return sum(p.astype(f32) for p in parts).astype(bf16)


def mp_sum(oth, own):
    chip = add(own(), lax.ppermute(oth, "c", SWAP))
    far = lax.ppermute(chip, "yl", SWAP)
    far_c = lax.ppermute(far, "c", SWAP)
    return chip, far, lax.ppermute(chip, "c", SWAP), far_c


def shards(z_star, cotangent, w_qkv, w_out):
    images, tokens, narrow = z_star.shape
    width = 4 * narrow
    heads = narrow // HD
    nx, ny, nz = [lax.axis_size(a) for a in DP]

    wide = like((tokens, width), bf16)
    wide_f = like((tokens, width), f32)
    half = like((tokens, 2 * narrow), bf16)
    g_like = like((tokens, 3 * narrow), bf16)
    proj = 2 * tokens * width * narrow
    small = 2 * tokens * tokens * HD * heads

    z0 = z_star[0]
    zy = lax.ppermute(z0, "yl", SWAP)
    zc = lax.ppermute(z0, "c", SWAP)
    t0, w = call(
        prepare_body,
        (like((tokens, narrow), bf16), like((3 * narrow, width), bf16)),
        (cotangent[0], jnp.swapaxes(w_qkv, 1, 2)),
        flops=proj,
    )
    (wo,) = call(prepare_out_body, (like((narrow, width), bf16),), (w_out,), flops=proj)
    tc = lax.ppermute(t0, "c", SWAP)
    zcy = lax.ppermute(zy, "c", SWAP)
    ty = lax.ppermute(t0, "yl", SWAP)
    tcy = lax.ppermute(ty, "c", SWAP)
    normal, xt, inv, qkv, probs, att = call(
        forward_body,
        (
            wide,
            like((width, tokens), bf16),
            like((tokens, 128), f32),
            like((3 * heads, tokens, HD), bf16),
            like((heads, tokens, tokens), f32),
            like((tokens, narrow), bf16),
        ),
        (z0, zy, zc, zcy, w),
        [pltpu.VMEM((tokens, width), bf16)],
        flops=3 * proj + 2 * small,
    )

    def own_of(grads):
        return call(own_body, (half,), (grads, w), flops=3 * proj // 2)[0]

    cot, grads, oth = call(
        first_body,
        (wide, g_like, half),
        (t0, ty, tc, tcy, wo, qkv, probs, w),
        flops=3 * proj + 4 * small,
    )
    sums = mp_sum(oth, lambda: own_of(grads))
    term, grads, oth = call(
        middle_body,
        (wide_f, g_like, half),
        (*sums, normal, inv, wo, qkv, probs, w),
        flops=3 * proj + 4 * small,
    )
    sums = mp_sum(oth, lambda: own_of(grads))

    rows = width // (nx * ny)
    each = rows // nz
    tall = pltpu.VMEM((4 * rows, tokens), bf16)
    tall_like = like((4 * rows, tokens), bf16)
    one, two, three = 512, 448, narrow
    give_one = ((1, 0), (1, 1), (2, 0), (2, 1))
    keep_one = ((0, 0), (0, 1), (3, 0), (3, 1))
    give_two = ((3, 0), (2, 0), (3, 1), (2, 1))
    keep_two = ((0, 0), (1, 0), (0, 1), (1, 1))
    give_three = ((0, 1), (3, 1), (1, 1), (2, 1))
    keep_three = ((0, 0), (3, 0), (1, 0), (2, 0))

    def swap_x(value, by):
        return lax.ppermute(value, "x", [(i, i ^ by) for i in range(nx)])

    def swap_yh(value):
        return lax.ppermute(value, "yh", SWAP)

    def pick(picks):
        body = functools.partial(pick_body, picks)
        (part,) = call(body, (tall_like,), (xt,), flops=proj)
        return part

    x_two = swap_x(pick(give_two), 3)
    x_one = swap_x(pick(give_one), 1)

    implicit, total, tt, s3 = call(
        functools.partial(total_body, give_three),
        (
            like((tokens, narrow), f32),
            wide,
            like((width, tokens), bf16),
            like((4 * folded(three), LANES), bf16),
        ),
        (*sums, normal, inv, cot, term, cotangent[0], att),
        [pltpu.VMEM((tokens, width), f32), tall],
        flops=proj,
    )
    g3 = swap_yh(s3)
    g_one, g_two = call(
        last_body,
        (like((tokens, one), bf16), like((tokens, two), bf16)),
        (total, wo, qkv, probs),
        [pltpu.VMEM((tokens, 3 * narrow), bf16)],
        flops=proj + 4 * small,
    )
    p_two = swap_x(g_two, 3)
    p_one = swap_x(g_one, 1)

    def block(picks, x, g, dtype):
        cols = g.shape[1]
        return call(
            functools.partial(rows_body, picks),
            (like((4 * rows, cols), dtype),),
            (x, g),
            [tall],
            flops=2 * tokens * 4 * rows * cols,
        )[0]

    def both(start, mine, x, g):
        return call(
            functools.partial(both_body, start * rows),
            (like((2 * folded(g.shape[1]), LANES), bf16),),
            (mine, x, g),
            flops=2 * tokens * 2 * rows * g.shape[1],
        )[0]

    m2 = block(keep_two, xt, g_two, f32)
    m1 = block(keep_one, xt, g_one, f32)
    (k3,) = call(
        functools.partial(folded_rows_body, keep_three),
        (like((4 * folded(three), LANES), bf16),),
        (tt, att),
        [tall],
        flops=2 * tokens * 4 * rows * three,
    )

    def at(value, start, count, parts):
        size = value.shape[0] // parts
        return value[start * size : (start + count) * size]

    h2 = swap_yh(both(2, m2, x_two, p_two))
    h1 = swap_x(both(2, m1, x_one, p_one), 3)
    h3 = swap_x(add(at(k3, 2, 2, 4), at(g3, 2, 2, 4)), 1)
    k2 = both(0, m2, x_two, p_two)
    k1 = both(0, m1, x_one, p_one)
    k3 = add(at(k3, 0, 2, 4), at(g3, 0, 2, 4))

    def last_half(k, h, swap):
        got = swap(add(at(k, 1, 1, 2), at(h, 1, 1, 2)))
        return add(at(k, 0, 1, 2), at(h, 0, 1, 2)), got

    e2 = last_half(k2, h2, lambda v: swap_x(v, 1))
    e1 = last_half(k1, h1, swap_yh)
    e3 = last_half(k3, h3, lambda v: swap_x(v, 3))
    dense = each * width // 128
    (packed,) = call(
        functools.partial(pack_body, (one, two, three)),
        (like((nz, dense, 128), bf16),),
        (*e1, *e2, *e3),
        [pltpu.VMEM((rows, width), f32)],
        flops=rows * width,
    )
    got = lax.all_to_all(packed, "z", 0, 0, tiled=True)
    factor = 1.0 / math.sqrt(images * nx * ny * nz * tokens)
    grad_qkv, grad_o = call(
        functools.partial(unpack_body, factor),
        (like((3, each, narrow), f32), like((each, narrow), f32)),
        (got,),
        [pltpu.VMEM((each, width), f32)],
        flops=rows * width,
    )
    return implicit[None], grad_qkv, grad_o.T


def solution(mesh):
    split = Mesh(mesh.devices.reshape(4, 2, 8, 2, 2), AXES)

    return jax.shard_map(
        shards,
        mesh=split,
        in_specs=(P(DP, None, MP), P(DP, None, MP), P(None, None, MP), P(MP, None)),
        out_specs=(P(DP, None, MP), P(None, DP, MP), P(MP, DP)),
        check_vma=False,
    )
```
